256 devices in a mesh: groups: 4 (over x, y), img: 32 (over z), space: 2 (over core).
Axes of the slice: x: 2, y: 2, z: 32, core: 2. Of those that a mesh axis runs over, the one named last changes fastest.
The devices are a block of a 4x8x32 slice.
Arguments:
- path: float32 [512, 64, 4096], P(('groups', 'img'), 'space'), parts along dimension 0, may hold values from -3 to 3
- bracket: int32 [512], P(('groups', 'img')), parts along dimension 0, may hold values from 0 to 126, as said below
Outputs:
- new_path: float32 [512, 64, 4096], P(('groups', 'img'), 'space'), parts along dimension 0
The draws below stay inside these ranges and needn't reach their ends.
There are 4 independent parts, one for each index of `groups`. The reference program is written for one: setup_inputs(seed, part) draws one part's arguments, and reference() takes and returns one part's arrays. A program takes and returns all parts, laid end to end along the dimension named above; each array names one. Nothing has to cross between parts.
Inputs may be any that keep to these rules, and one draw needn't show every extreme that they name: bracket[j] differs from j by at most 2; it is given, not derived from the arc lengths, so the target arc length of image j need not lie between arc_b and arc_(b+1).
All inputs are finite; a program needn't handle non-finite values.
Results may differ from the reference program's by a relative error of at most 0.0003.
Values sent between devices are 32-bit elements; how exact they have to be, the bound alone decides.
A program may use at most 64 MiB of HBM per device.

```python
import jax
import jax.numpy as jnp
from jax import lax

COLS = 4096
REACH = 2
ITERS = 2
IMAGES = 128
GRID_ROWS = 64


def draw_bracket(key, part):
    offsets = jax.random.randint(jax.random.fold_in(key, 7), (IMAGES,), -REACH, REACH + 1)
    return jnp.clip(jnp.arange(IMAGES) + offsets, 0, IMAGES - 2).astype(jnp.int32)


def levels(rng, extent, pieces, smallest, high):
    loudness = 1.0
    for position, parts in pieces:
        steps = jax.random.uniform(jax.random.fold_in(jax.random.fold_in(rng, 6), position), (parts,), jnp.float32, smallest / len(pieces), high / len(pieces))
        loudness = loudness * jnp.repeat(jnp.exp(steps), extent[position] // parts).reshape((-1,) + (1,) * (len(extent) - 1 - position))
    return loudness


def bell_draw(own_key, dims, scale, limit, pieces=(), held_as=jnp.bfloat16):
    array = jax.random.normal(own_key, dims, jnp.float32) * scale
    if len(pieces) > 0:
        array = levels(own_key, dims, pieces, -0.22, 0.18) * array
    return jnp.clip(array, min=-limit, max=limit).astype(held_as)


def setup_inputs(seed: int = 0, part: int = 0) -> dict:
    keys = jax.random.split(jax.random.key(seed), 3)
    part_splits = jax.random.split(jax.random.fold_in(keys[2], part), 3)
    path = bell_draw(part_splits[0], (IMAGES, GRID_ROWS, COLS), 0.5, 3.0, ((0, 32), (1, 2)), jnp.float32)
    bracket = draw_bracket(jax.random.fold_in(jax.random.fold_in(keys[2], part), 71), part)
    return {"path": path, "bracket": bracket}


TIME_STEP = 0.002
EPSILON = 1e-06

def laplace(field):
    return jnp.roll(field, 1, -2) + jnp.roll(field, -1, -2) + jnp.roll(field, 1, -1) + jnp.roll(field, -1, -1) - 4.0 * field

def along_path(field, count):
    ids = jnp.arange(count)
    is_first = (ids == 0)[:, None, None]
    is_last = (ids == count - 1)[:, None, None]
    earlier = jnp.concatenate([field[:1], field[:-1]], axis=0)
    following = jnp.concatenate([field[1:], field[-1:]], axis=0)
    stretch = jnp.where(is_first | is_last, jnp.float32(count - 1), jnp.float32((count - 1) / 2.0))
    return (following - earlier) * stretch

def iterate(images, count):
    tangent = along_path(images, count)
    drift_v = laplace(images) + images - images ** 3
    speed = jnp.sqrt(lax.optimization_barrier(jnp.sum(drift_v * drift_v, axis=(1, 2))) + EPSILON) / jnp.sqrt(lax.optimization_barrier(jnp.sum(tangent * tangent, axis=(1, 2))) + EPSILON)
    theta = speed[:, None, None] * tangent - drift_v
    descent = speed[:, None, None] * along_path(theta, count) + laplace(theta) + (1.0 - 3.0 * images * images) * theta
    ids = jnp.arange(count)
    inside = ((ids > 0) & (ids < count - 1))[:, None, None]
    return images + TIME_STEP * jnp.where(inside, descent, 0.0)

def reference(path, bracket):
    count = path.shape[0]
    images = path
    for iteration in range(ITERS):
        images = iterate(images, count)
    diffs = images[1:] - images[:-1]
    segments = jnp.sqrt(lax.optimization_barrier(jnp.sum(diffs * diffs, axis=(1, 2))) + EPSILON)
    seg_full = jnp.concatenate([jnp.zeros((1,), segments.dtype), segments])
    arc = jnp.cumsum(seg_full)
    length = arc[-1]
    target = length * jnp.arange(count).astype(segments.dtype) / (count - 1)
    lower = bracket.astype(jnp.int32)
    weight = (target - arc[lower]) / seg_full[lower + 1]
    base = images[lower]
    return base + weight[:, None, None] * (images[lower + 1] - base)
```

```python
import functools

import jax
import jax.numpy as jnp
from jax import lax
from jax.experimental import pallas as pl
from jax.experimental.pallas import tpu as pltpu
from jax.sharding import PartitionSpec as P

REACH = 2
ITERS = 2
TIME_STEP = 0.002
EPSILON = 1e-06

LANES = 128
SUB = 8
OWN = 4
TILES = 4
EXT = TILES + 1
FIRST = 4
WINDOW = OWN + 2 * FIRST


def fold(block):
    parts = [block[:, i : i + LANES] for i in range(0, block.shape[1], LANES)]
    while len(parts) > 1:
        parts = [a + b for a, b in zip(parts[::2], parts[1::2])] + parts[len(parts) // 2 * 2 :]
    return parts[0]


def spread(vector, width):
    return jnp.concatenate([vector] * (width // LANES), axis=1)


def kernel(count, axes, path, bracket, out, phi0, phi1, phi2_0, phi2_1, phi2_2, phi2_3, th0, th1, rows_in, mine0, theirs0, mine1, theirs1,
           mine2, theirs2, speed0, speed1, message, gathered, result,
           local_sem, up_send, up_recv, down_send, down_recv, row_send, row_recv, sum_send, sum_recv,
           new_send, new_recv, len_send, len_recv, out_sem, live):
    cols = path.shape[-1]
    half = min(cols, 1024)
    phi2 = (phi2_0, phi2_1, phi2_2, phi2_3)
    img = lax.axis_index("img")
    core = lax.axis_index("space")

    low = lax.rem(img + count - 1, count)
    high = lax.rem(img + 1, count)
    partner = 1 - core
    to_low, to_high, to_partner = {"img": low}, {"img": high}, {"space": partner}
    mesh_id = pl.DeviceIdType.MESH

    def remote(src, dst, send, recv, where):
        return pltpu.make_async_remote_copy(
            src_ref=src, dst_ref=dst, send_sem=send, recv_sem=recv, device_id=where, device_id_type=mesh_id
        )

    loads = [
        pltpu.make_async_copy(path.at[i], phi0.at[FIRST + i, pl.ds(0, TILES)], local_sem.at[i]) for i in range(OWN)
    ]
    for i in (0, 3, 1, 2):
        loads[i].start()

    barrier = pltpu.get_barrier_semaphore()
    for where in (to_low, to_high, to_partner):
        pl.semaphore_signal(barrier, inc=1, device_id=where, device_id_type=mesh_id)
    pl.semaphore_wait(barrier, 3)

    own = lambda image: phi0.at[image, pl.ds(0, TILES)]
    down = [
        remote(own(FIRST + i), own(FIRST + OWN + i), down_send.at[i], down_recv.at[i], to_low) for i in range(OWN)
    ]
    up = [remote(own(FIRST + i), own(i), up_send.at[i], up_recv.at[i], to_high) for i in range(OWN)]

    def row_copies(image):
        return [
            remote(phi0.at[image, tile], rows_in.at[image, k], row_send.at[image, k], row_recv.at[image, k], to_partner)
            for k, tile in enumerate((0, TILES - 1))
        ]

    row_moves = {image: row_copies(image) for image in range(1, WINDOW - 1)}

    for i in (0, 3, 1, 2):
        loads[i].wait()
        if i == 0:
            down[0].start()
        elif i == 3:
            up[3].start()
    for i in range(1, OWN):
        down[i].start()
        up[OWN - 1 - i].start()
    for image in range(FIRST, FIRST + OWN):
        for copy in row_moves[image]:
            copy.start()
    far = 1
    step = 0
    lives = []
    while 2 * far < count + 1 and far < count // 2:
        lives.append(far)
        far *= 2

    def say_live(step):
        distance = lives[step]
        for other in (lax.rem(img + distance, count), lax.rem(img + count - distance, count)):
            pl.semaphore_signal(live.at[step], inc=1, device_id={"img": other}, device_id_type=mesh_id)

    def hear_live(step):
        pl.semaphore_wait(live.at[step], 2)

    if lives:
        say_live(0)

    sub = lax.broadcasted_iota(jnp.int32, (SUB, half), 0)
    chunks = range(0, cols, half)

    is_first = (img == 0).astype(jnp.int32)
    is_last = (img == count - 1).astype(jnp.int32)
    last = OWN * count - 1

    def sides(image):
        at_first = is_first * (image == FIRST).astype(jnp.int32)
        at_last = is_last * (image == FIRST + OWN - 1).astype(jnp.int32)
        end = (at_first + at_last).astype(jnp.float32)
        return image - 1 + at_first, image + 1 - at_last, (1.0 + end) * jnp.float32(last / 2.0)

    def around(ref, slot, tile, c):
        above = lax.rem(tile + EXT - 1, EXT)
        below = lax.rem(tile + 1, EXT)
        here = ref[slot, tile, :, c : c + half]
        up_rows = pltpu.roll(jnp.where(sub == SUB - 1, ref[slot, above, :, c : c + half], here), 1, 0)
        down_rows = pltpu.roll(jnp.where(sub == 0, ref[slot, below, :, c : c + half], here), SUB - 1, 0)
        if half == cols:
            left = pltpu.roll(here, 1, 1)
            right = pltpu.roll(here, half - 1, 1)
        else:
            before = (c - LANES) % cols
            after = (c + half) % cols
            wide = jnp.concatenate(
                [ref[slot, tile, :, before : before + LANES], here, ref[slot, tile, :, after : after + LANES]], axis=1
            )
            left = pltpu.roll(wide, 1, 1)[:, LANES : LANES + half]
            right = pltpu.roll(wide, half + 2 * LANES - 1, 1)[:, LANES : LANES + half]
        return here, (up_rows + down_rows) + (left + right) - 4.0 * here

    zero = jnp.zeros((SUB, LANES), jnp.float32)

    def make_halo(image):
        for c in chunks:
            phi0[image, TILES, :, c : c + half] = jnp.where(
                sub < SUB // 2, rows_in[image, 0, :, c : c + half], rows_in[image, 1, :, c : c + half]
            )

    def drift(phi, th, slot, th_slot, tiles, total):
        def one(tile, acc):
            for c in chunks:
                here, lap = around(phi, slot, tile, c)
                force = lap + here - here * here * here
                th[th_slot, tile, :, c : c + half] = force
                acc = acc + jnp.where(tile < TILES, fold(force * force), 0.0)
            return acc

        total[...] = lax.fori_loop(0, tiles, one, zero)

    def stretch_sum(phi, lower, upper, total, factor):
        def one(tile, acc):
            for c in chunks:
                gap = phi[upper, tile, :, c : c + half] - phi[lower, tile, :, c : c + half]
                acc = acc + fold(gap * gap)
            return acc

        total[...] = lax.fori_loop(0, TILES, one, zero) * (factor * factor)

    def segment_sum(upper, total):
        acc = zero
        for ref in phi2:
            for c in chunks:
                gap = ref[upper, :, c : c + half] - ref[upper - 1, :, c : c + half]
                acc = acc + fold(gap * gap)
        total[...] = acc

    def theta(phi, th, lower, upper, factor, th_slot, speed, tiles):
        scale = spread(speed * factor, half)

        def one(tile, carry):
            for c in chunks:
                span = slice(c, c + half)
                gap = phi[upper, tile, :, span] - phi[lower, tile, :, span]
                th[th_slot, tile, :, span] = scale * gap - th[th_slot, tile, :, span]
            return carry

        lax.fori_loop(0, tiles, one, 0)

    def advance(phi, slot, th, th_slot, new, new_slot, speed, image, tiles):
        fixed = is_first * (image == FIRST).astype(jnp.int32) + is_last * (image == FIRST + OWN - 1).astype(jnp.int32)
        scale = spread(speed * jnp.float32(last / 2.0), half)

        def one(tile, carry):
            for c in chunks:
                span = slice(c, c + half)
                here, lap = around(th, th_slot, tile, c)
                old = phi[slot, tile, :, span]
                bend = th[th_slot + 1, tile, :, span] - th[th_slot - 1, tile, :, span]
                descent = scale * bend + lap + (1.0 - 3.0 * old * old) * here
                value = jnp.where(fixed == 0, old + TIME_STEP * descent, old)
                if new is phi2:
                    new[tile][new_slot, :, span] = value
                else:
                    new[new_slot, tile, :, span] = value
            return carry

        if new is phi2:
            for tile in range(tiles):
                one(tile, 0)
        else:
            lax.fori_loop(0, tiles, one, 0)

    def whole(a):
        return jnp.broadcast_to(jnp.sum(jnp.sum(a, axis=1, keepdims=True), axis=0, keepdims=True), (SUB, LANES))

    def speeds(mine, theirs, first, number, out_ref):
        for i in range(first, first + number):
            force = whole(mine[i, 0] + theirs[i, 0])
            stretch = whole(mine[i, 1] + theirs[i, 1])
            out_ref[i] = jnp.sqrt(force + EPSILON) / jnp.sqrt(stretch + EPSILON)

    def swap(mine, theirs, first, number, k):
        span = pl.ds(first, number)
        return remote(mine.at[span], theirs.at[span], sum_send.at[k], sum_recv.at[k], to_partner)

    p1, t0, t1 = lambda w: w - 2, lambda w: w - 1, lambda w: w - 3

    def place_of(image):
        outer_low = OWN + 2 * (FIRST - 1 - image)
        outer_high = OWN + 2 * (image - FIRST - OWN) + 1
        return jnp.where(image < FIRST, outer_low, jnp.where(image < FIRST + OWN, image - FIRST, outer_high))

    def each(images, body):
        start, step, number = images

        def one(i, carry):
            image = start + step * i
            body(image, place_of(image))
            return carry

        lax.fori_loop(0, number, one, 0)

    every = (FIRST, 1, OWN)
    inner = (FIRST + 1, 1, OWN - 2)

    def pair(n):
        return (FIRST - n, 2 * n + OWN - 1, 2)

    def pair_in(n):
        return pair(n - 1) if n > 1 else (FIRST, OWN - 1, 2)

    def gap0(image, place):
        lower, upper, factor = sides(image)
        stretch_sum(phi0, lower, upper, mine0.at[place, 1], factor)

    def drift0(tiles):
        def body(image, place):
            drift(phi0, th0, image, t0(image), tiles, mine0.at[place, 0])

        return body

    def theta0(tiles):
        def body(image, place):
            lower, upper, factor = sides(image)
            theta(phi0, th0, lower, upper, factor, t0(image), speed0[place], tiles)

        return body

    def next1(tiles):
        def body(image, _):
            advance(phi0, image, th0, t0(image), phi1, p1(image), speed0[place_of(image)], image, tiles)

        return body

    def gap1(image, _):
        lower, upper, factor = sides(image)
        stretch_sum(phi1, p1(lower), p1(upper), mine1.at[place_of(image), 1], factor)

    def drift1(tiles):
        def body(image, _):
            drift(phi1, th1, p1(image), t1(image), tiles, mine1.at[place_of(image), 0])

        return body

    def theta1(tiles):
        def body(image, _):
            lower, upper, factor = sides(image)
            theta(phi1, th1, p1(lower), p1(upper), factor, t1(image), speed1[place_of(image)], tiles)

        return body

    def next2(image, _):
        advance(phi1, p1(image), th1, t1(image), phi2, image - 2, speed1[place_of(image)], image, TILES)

    def arrive(n):
        down[n - 1].wait_recv()
        up[OWN - n].wait_recv()

    def halo(images):
        for image in images:
            for copy in row_moves[image]:
                copy.wait_recv()
            make_halo(image)

    halo(range(FIRST, FIRST + OWN))
    each(every, drift0(EXT))
    each(inner, gap0)

    swaps = []

    def exchange(mine, theirs, first, number):
        move = swap(mine, theirs, first, number, len(swaps))
        move.start()
        swaps.append(move)
        return move

    for n in range(1, FIRST + 1):
        outer = (FIRST - n, FIRST + OWN - 1 + n)
        arrive(n)
        if n < FIRST:
            for image in outer:
                for copy in row_moves[image]:
                    copy.start()
        each(pair_in(n), gap0)
        first, number = (0, OWN) if n == 1 else (OWN + 2 * (n - 2), 2)
        move = exchange(mine0, theirs0, first, number)
        if n < FIRST:
            halo(outer)
        move.wait_recv()
        speeds(mine0, theirs0, first, number, speed0)
        if n == 1:
            each(every, theta0(EXT))
            each(inner, next1(EXT))
        else:
            each(pair_in(n), theta0(EXT if n < FIRST else TILES))
            each(pair_in(n - 1), next1(EXT if n < FIRST else TILES))
        if n == 2:
            each(every, drift1(EXT))
            each(inner, gap1)
        if n >= 3:
            each(pair_in(n - 2), gap1)
            first, number = (0, OWN) if n == 3 else (OWN, 2)
            move = exchange(mine1, theirs1, first, number)
            move.wait_recv()
            speeds(mine1, theirs1, first, number, speed1)
            if n == 3:
                each(every, theta1(EXT))
                each(inner, next2)
            else:
                each(pair_in(2), theta1(TILES))
                each(pair_in(1), next2)
        if n == 3:
            down_new = []
            for k, (source, target) in enumerate(((5, 9), (6, 10), (4, 8))):
                down_new.append([
                    remote(phi2[t].at[source - 2], phi2[t].at[target - 2], new_send.at[k, t], new_recv.at[k, t], to_low)
                    for t in range(TILES)
                ])
            up_new = []
            for k, (source, target) in enumerate(((7, 3), (6, 2))):
                up_new.append([
                    remote(phi2[t].at[source - 2], phi2[t].at[target - 2], new_send.at[3 + k, t],
                           new_recv.at[3 + k, t], to_high)
                    for t in range(TILES)
                ])
            for k in (0, 1):
                for copy in down_new[k]:
                    copy.start()
        if n < FIRST:
            each(pair(n), drift0(EXT if n < FIRST - 1 else TILES))
        if n == 3:
            each(pair(1), drift1(TILES))
        if n <= len(lives):
            hear_live(n - 1)
            if n < len(lives):
                say_live(n)

    for k in (0, 1):
        for copy in up_new[k]:
            copy.start()
    for image in range(FIRST + 1, FIRST + OWN):
        segment_sum(image - 2, mine2.at[image - FIRST])
    for copy in up_new[0]:
        copy.wait_recv()
    segment_sum(2, mine2.at[0])
    move = exchange(mine2, theirs2, 0, OWN)
    move.wait_recv()

    lane = lax.broadcasted_iota(jnp.int32, (1, LANES), 1)
    lengths = jnp.zeros((1, LANES), jnp.float32)
    for i in range(OWN):
        segment = jnp.sqrt(whole(mine2[i] + theirs2[i])[0:1] + EPSILON)
        if i == 0:
            segment = jnp.where(img == 0, 0.0, segment)
        lengths = jnp.where(lane == i, segment, lengths)
    message[0] = lengths
    gathered[img] = lengths

    def send_length(k):
        return remote(message.at[0], gathered.at[img], len_send.at[k], len_recv.at[k], {"img": lax.rem(img + k, count)})

    def spread_out(i, carry):
        distance = count // 2 - 1 - i
        send_length(distance).start()
        send_length(count - distance).start()
        return carry

    send_length(count // 2).start()
    lax.fori_loop(0, count // 2 - 1, spread_out, 0)
    for copy in down_new[2]:
        copy.start()

    def heard(k, carry):
        send_length(k).wait_recv()
        return carry

    lax.fori_loop(1, count, heard, 0)

    owner = lax.broadcasted_iota(jnp.int32, (count, 1, LANES), 0)
    place = lax.broadcasted_iota(jnp.int32, (count, 1, LANES), 2)
    index = OWN * owner + place
    segs = jnp.where(place < OWN, gathered[...], 0.0)

    def add_up(a):
        return jnp.sum(jnp.sum(a, axis=0), axis=1, keepdims=True)

    length = add_up(segs)
    weights = []
    for i in range(OWN):
        base = bracket[i]
        arc = add_up(jnp.where(index <= base, segs, 0.0))
        seg = add_up(jnp.where(index == base + 1, segs, 0.0))
        target = length * (OWN * img + i).astype(jnp.float32) / jnp.float32(last)
        weights.append(jnp.broadcast_to((target - arc) / seg, (SUB, half)))

    writes = [pltpu.make_async_copy(result.at[t], out.at[t], out_sem.at[t]) for t in range(TILES)]
    for t in range(TILES):
        for k in (0, 1, 2):
            down_new[k][t].wait_recv()
        if t == 0:
            for copy in up_new[1]:
                copy.wait_recv()
        for i in range(OWN):
            pick = jnp.clip(bracket[i] - (OWN * img - 2), 0, WINDOW - 5)
            for c in chunks:
                span = slice(c, c + half)
                base = phi2[t][pick, :, span]
                result[t, i, :, span] = base + weights[i] * (phi2[t][pick + 1, :, span] - base)
        writes[t].start()

    for copy in down + up:
        copy.wait_send()
    for image in row_moves:
        for copy in row_moves[image]:
            copy.wait_send()
    for move in swaps:
        move.wait_send()
    for group in down_new + up_new:
        for copy in group:
            copy.wait_send()

    def sent(k, carry):
        send_length(k).wait_send()
        return carry

    lax.fori_loop(1, count, sent, 0)
    for copy in writes:
        copy.wait()


def per_device(count, axes, path, bracket):
    images, rows, cols = path.shape
    f32 = jnp.float32
    dma = pltpu.SemaphoreType.DMA
    tiled = path.reshape(images, TILES, SUB, cols)
    out = pl.pallas_call(
        functools.partial(kernel, count, axes),
        out_shape=jax.ShapeDtypeStruct((TILES, images, SUB, cols), f32),
        in_specs=[pl.BlockSpec(memory_space=pl.ANY), pl.BlockSpec(memory_space=pltpu.SMEM)],
        out_specs=pl.BlockSpec(memory_space=pl.ANY),
        scratch_shapes=[
            pltpu.VMEM((WINDOW, EXT, SUB, cols), f32),
            pltpu.VMEM((WINDOW - 4, EXT, SUB, cols), f32),
            *[pltpu.VMEM((WINDOW - 3, SUB, cols), f32) for _ in range(TILES)],
            pltpu.VMEM((WINDOW - 2, EXT, SUB, cols), f32),
            pltpu.VMEM((WINDOW - 6, EXT, SUB, cols), f32),
            pltpu.VMEM((WINDOW, 2, SUB, cols), f32),
            pltpu.VMEM((WINDOW, 2, SUB, LANES), f32),
            pltpu.VMEM((WINDOW, 2, SUB, LANES), f32),
            pltpu.VMEM((OWN + 2, 2, SUB, LANES), f32),
            pltpu.VMEM((OWN + 2, 2, SUB, LANES), f32),
            pltpu.VMEM((OWN, SUB, LANES), f32),
            pltpu.VMEM((OWN, SUB, LANES), f32),
            pltpu.VMEM((WINDOW, SUB, LANES), f32),
            pltpu.VMEM((WINDOW, SUB, LANES), f32),
            pltpu.VMEM((1, 1, LANES), f32),
            pltpu.VMEM((count, 1, LANES), f32),
            pltpu.VMEM((TILES, images, SUB, cols), f32),
            dma((OWN,)),
            dma((OWN,)),
            dma((OWN,)),
            dma((OWN,)),
            dma((OWN,)),
            dma((WINDOW, 2)),
            dma((WINDOW, 2)),
            dma((8,)),
            dma((8,)),
            dma((5, TILES)),
            dma((5, TILES)),
            dma((count,)),
            dma((count,)),
            dma((TILES,)),
            pltpu.SemaphoreType.REGULAR((8,)),
        ],
        compiler_params=pltpu.CompilerParams(
            collective_id=0, has_side_effects=True, vmem_limit_bytes=62 * 1024 * 1024
        ),
    )(tiled, bracket)
    return out.transpose(1, 0, 2, 3).reshape(images, rows, cols)


def solution(mesh):
    count = mesh.shape["img"]
    return jax.shard_map(
        functools.partial(per_device, count, tuple(mesh.axis_names)),
        mesh=mesh,
        in_specs=(P(("groups", "img"), "space", None), P(("groups", "img"))),
        out_specs=P(("groups", "img"), "space", None),
        check_vma=False,
    )
```

```python
import functools

import jax
import jax.numpy as jnp
from jax import lax
from jax.experimental import pallas as pl
from jax.experimental.pallas import tpu as pltpu
from jax.sharding import PartitionSpec as P

REACH = 2
ITERS = 2
TIME_STEP = 0.002
EPSILON = 1e-06

LANES = 128
SUB = 8
OWN = 4
TILES = 4
EXT = TILES + 1
FIRST = 4


def fold(block):
    parts = [block[:, i : i + LANES] for i in range(0, block.shape[1], LANES)]
    while len(parts) > 1:
        parts = [a + b for a, b in zip(parts[::2], parts[1::2])] + parts[len(parts) // 2 * 2 :]
    return parts[0]


def spread(vector, width):
    return jnp.concatenate([vector] * (width // LANES), axis=1)


def kernel(count, path, bracket, out, phi0, phi1, phi2_0, phi2_1, phi2_2, phi2_3, th0, th1, rows0, rows1,
           mine0, theirs0, mine1, theirs1, mine2, theirs2, speed0, speed1, message, gathered, result,
           local_sem, down_send, down_recv, up_send, up_recv, row_send, row_recv, sum_send, sum_recv,
           new_send, new_recv, pace_send, pace_recv, len_send, len_recv, out_sem, live):
    cols = path.shape[-1]
    half = min(cols, 1024)
    phi2 = (phi2_0, phi2_1, phi2_2, phi2_3)
    img = lax.axis_index("img")
    core = lax.axis_index("space")

    low = lax.rem(img + count - 1, count)
    high = lax.rem(img + 1, count)
    partner = 1 - core
    to_low, to_high, to_partner = {"img": low}, {"img": high}, {"space": partner}
    mesh_id = pl.DeviceIdType.MESH

    def remote(src, dst, send, recv, where):
        return pltpu.make_async_remote_copy(
            src_ref=src, dst_ref=dst, send_sem=send, recv_sem=recv, device_id=where, device_id_type=mesh_id
        )

    p0, p1, p2, t0, t1 = (lambda w, s=s: w - s for s in (2, 1, 2, 3, 2))

    loads = [
        pltpu.make_async_copy(path.at[i], phi0.at[p0(FIRST + i), pl.ds(0, TILES)], local_sem.at[i]) for i in range(OWN)
    ]
    for i in (0, 3, 1, 2):
        loads[i].start()

    barrier = pltpu.get_barrier_semaphore()
    for where in (to_low, to_high, to_partner):
        pl.semaphore_signal(barrier, inc=1, device_id=where, device_id_type=mesh_id)
    pl.semaphore_wait(barrier, 3)

    def part(ref, slot, first=0, number=TILES):
        return ref.at[slot, pl.ds(first, number)]

    def shift(ref, name, source, target, k, where, first=0, number=TILES):
        send, recv = (down_send, down_recv) if where is to_low else (up_send, up_recv)
        return remote(part(ref, name(source), first, number), part(ref, name(target), first, number),
                      send.at[k], recv.at[k], where)

    down = [
        shift(phi0, p0, 4, 8, 0, to_low), shift(phi0, p0, 5, 9, 1, to_low),
        shift(phi1, p1, 5, 9, 2, to_low), shift(phi1, p1, 4, 8, 3, to_low),
        shift(phi1, p1, 6, 10, 4, to_low, 2, 2), shift(phi1, p1, 6, 10, 5, to_low, 0, 2),
    ]
    up = [
        shift(phi0, p0, 7, 3, 0, to_high), shift(phi0, p0, 6, 2, 1, to_high),
        shift(phi1, p1, 6, 2, 2, to_high), shift(phi1, p1, 7, 3, 3, to_high),
        shift(phi1, p1, 5, 1, 4, to_high, 0, 2), shift(phi1, p1, 5, 1, 5, to_high, 2, 2),
    ]
    down_new = [
        [remote(phi2[t].at[p2(source)], phi2[t].at[p2(target)], new_send.at[k, t], new_recv.at[k, t], to_low)
         for t in range(TILES)]
        for k, (source, target) in enumerate(((5, 9), (6, 10)))
    ]
    up_new = [
        remote(phi2[t].at[p2(6)], phi2[t].at[p2(2)], new_send.at[2, t], new_recv.at[2, t], to_high)
        for t in range(TILES)
    ]

    row_moves = []

    def send_rows(ref, slot, rows):
        copies = []
        for k, tile in enumerate((0, TILES - 1)):
            n = len(row_moves)
            copy = remote(ref.at[slot, tile], rows.at[slot, k], row_send.at[n], row_recv.at[n], to_partner)
            copy.start()
            row_moves.append(copy)
            copies.append(copy)
        return copies

    def halo(ref, slot, rows, copies):
        for copy in copies:
            copy.wait_recv()
        for c in chunks:
            ref[slot, TILES, :, c : c + half] = jnp.where(
                sub < SUB // 2, rows[slot, 0, :, c : c + half], rows[slot, 1, :, c : c + half]
            )

    sub = lax.broadcasted_iota(jnp.int32, (SUB, half), 0)
    chunks = range(0, cols, half)

    for i in (0, 3, 1, 2):
        loads[i].wait()
        if i == 0:
            down[0].start()
        elif i == 3:
            up[0].start()
        elif i == 1:
            down[1].start()
        else:
            up[1].start()
    own_rows = [send_rows(phi0, p0(image), rows0) for image in range(FIRST, FIRST + OWN)]
    far = 1
    step = 0
    lives = []
    while 2 * far < count + 1 and far < count // 2:
        lives.append(far)
        far *= 2

    def say_live(step):
        distance = lives[step]
        for other in (lax.rem(img + distance, count), lax.rem(img + count - distance, count)):
            pl.semaphore_signal(live.at[step], inc=1, device_id={"img": other}, device_id_type=mesh_id)

    def hear_live(step):
        pl.semaphore_wait(live.at[step], 2)

    if lives:
        say_live(0)

    is_first = (img == 0).astype(jnp.int32)
    is_last = (img == count - 1).astype(jnp.int32)
    last = OWN * count - 1

    def same(image, k):
        return jnp.asarray(image == k).astype(jnp.int32)

    def sides(image):
        at_first = is_first * same(image, FIRST)
        at_last = is_last * same(image, FIRST + OWN - 1)
        end = (at_first + at_last).astype(jnp.float32)
        return image - 1 + at_first, image + 1 - at_last, (1.0 + end) * jnp.float32(last / 2.0)

    def around(ref, slot, tile, c):
        above = lax.rem(tile + EXT - 1, EXT)
        below = lax.rem(tile + 1, EXT)
        here = ref[slot, tile, :, c : c + half]
        up_rows = pltpu.roll(jnp.where(sub == SUB - 1, ref[slot, above, :, c : c + half], here), 1, 0)
        down_rows = pltpu.roll(jnp.where(sub == 0, ref[slot, below, :, c : c + half], here), SUB - 1, 0)
        if half == cols:
            left = pltpu.roll(here, 1, 1)
            right = pltpu.roll(here, half - 1, 1)
        else:
            before = (c - LANES) % cols
            after = (c + half) % cols
            wide = jnp.concatenate(
                [ref[slot, tile, :, before : before + LANES], here, ref[slot, tile, :, after : after + LANES]], axis=1
            )
            left = pltpu.roll(wide, 1, 1)[:, LANES : LANES + half]
            right = pltpu.roll(wide, half + 2 * LANES - 1, 1)[:, LANES : LANES + half]
        return here, (up_rows + down_rows) + (left + right) - 4.0 * here

    zero = jnp.zeros((SUB, LANES), jnp.float32)

    def over(tiles, one, init):
        first, end = tiles
        return lax.fori_loop(first, end, one, init)

    full, slab, upper_half, lower_half = (0, EXT), (0, TILES), (0, 2), (2, TILES)

    def drift(phi, th, slot, th_slot, tiles, total=None):
        def one(tile, acc):
            for c in chunks:
                here, lap = around(phi, slot, tile, c)
                force = lap + here - here * here * here
                th[th_slot, tile, :, c : c + half] = force
                acc = acc + jnp.where(tile < TILES, fold(force * force), 0.0)
            return acc

        acc = over(tiles, one, zero)
        if total is not None:
            total[...] = acc

    def stretch_sum(phi, lower, upper, total, factor):
        def one(tile, acc):
            for c in chunks:
                gap = phi[upper, tile, :, c : c + half] - phi[lower, tile, :, c : c + half]
                acc = acc + fold(gap * gap)
            return acc

        total[...] = over(slab, one, zero) * (factor * factor)

    def segment_sum(image, total, tiles=range(TILES)):
        acc = zero
        for t in tiles:
            for c in chunks:
                gap = phi2[t][p2(image), :, c : c + half] - phi2[t][p2(image - 1), :, c : c + half]
                acc = acc + fold(gap * gap)
        total[...] = acc

    def theta(phi, th, lower, upper, factor, th_slot, speed, tiles):
        scale = spread(speed * factor, half)

        def one(tile, carry):
            for c in chunks:
                span = slice(c, c + half)
                gap = phi[upper, tile, :, span] - phi[lower, tile, :, span]
                th[th_slot, tile, :, span] = scale * gap - th[th_slot, tile, :, span]
            return carry

        over(tiles, one, 0)

    def advance(phi, slot, th, th_slot, new, new_slot, speed, image, tiles):
        fixed = is_first * same(image, FIRST) + is_last * same(image, FIRST + OWN - 1)
        scale = spread(speed * jnp.float32(last / 2.0), half)

        def one(tile, carry):
            for c in chunks:
                span = slice(c, c + half)
                here, lap = around(th, th_slot, tile, c)
                old = phi[slot, tile, :, span]
                bend = th[th_slot + 1, tile, :, span] - th[th_slot - 1, tile, :, span]
                descent = scale * bend + lap + (1.0 - 3.0 * old * old) * here
                value = jnp.where(fixed == 0, old + TIME_STEP * descent, old)
                if new is phi2:
                    new[tile][new_slot, :, span] = value
                else:
                    new[new_slot, tile, :, span] = value
            return carry

        if new is phi2:
            for tile in range(*tiles):
                one(tile, 0)
        else:
            over(tiles, one, 0)

    def whole(a):
        return jnp.broadcast_to(jnp.sum(jnp.sum(a, axis=1, keepdims=True), axis=0, keepdims=True), (SUB, LANES))

    def speeds(mine, theirs, first, number, out_ref):
        for i in range(first, first + number):
            force = whole(mine[i, 0] + theirs[i, 0])
            stretch = whole(mine[i, 1] + theirs[i, 1])
            out_ref[i] = jnp.sqrt(force + EPSILON) / jnp.sqrt(stretch + EPSILON)

    def place(image):
        if isinstance(image, int):
            return 2 * (5 - image) if image < 6 else 2 * (image - 6) + 1
        return jnp.where(image < 6, 2 * (5 - image), 2 * (image - 6) + 1)

    def each(images, body):
        start, step, number = images

        def one(i, carry):
            body(start + step * i)
            return carry

        lax.fori_loop(0, number, one, 0)

    every, mids, ends, outs = (4, 1, 4), (5, 1, 2), (4, 3, 2), (3, 5, 2)

    def gap0(image):
        lower, upper, factor = sides(image)
        stretch_sum(phi0, p0(lower), p0(upper), mine0.at[place(image), 1], factor)

    def drift0(image):
        drift(phi0, th0, p0(image), t0(image), full, mine0.at[place(image), 0])

    def theta0(image):
        lower, upper, factor = sides(image)
        theta(phi0, th0, p0(lower), p0(upper), factor, t0(image), speed0[place(image)], full)

    def next1(image):
        advance(phi0, p0(image), th0, t0(image), phi1, p1(image), speed0[place(image)], image, full)

    def gap1(image):
        lower, upper, factor = sides(image)
        stretch_sum(phi1, p1(lower), p1(upper), mine1.at[place(image), 1], factor)

    def drift1(image):
        drift(phi1, th1, p1(image), t1(image), full, mine1.at[place(image), 0])

    def theta1(image, tiles=full):
        lower, upper, factor = sides(image)
        theta(phi1, th1, p1(lower), p1(upper), factor, t1(image), speed1[place(image)], tiles)

    def next2(image, tiles=slab):
        advance(phi1, p1(image), th1, t1(image), phi2, p2(image), speed1[place(image)], image, tiles)

    swaps = []

    def exchange(mine, theirs, first, number):
        k = len(swaps)
        span = pl.ds(first, number)
        move = remote(mine.at[span], theirs.at[span], sum_send.at[k], sum_recv.at[k], to_partner)
        move.start()
        swaps.append(move)
        return move

    def arrive(k):
        down[k].wait_recv()
        up[k].wait_recv()

    def live_round(n):
        if n < len(lives):
            hear_live(n)
            if n + 1 < len(lives):
                say_live(n + 1)

    for image in range(FIRST, FIRST + OWN):
        halo(phi0, p0(image), rows0, own_rows[image - FIRST])
    each(every, drift0)
    each(mids, gap0)

    arrive(0)
    rows = {image: send_rows(phi0, p0(image), rows0) for image in (3, 8)}
    each(ends, gap0)
    move = exchange(mine0, theirs0, 0, OWN)
    for image in (3, 8):
        halo(phi0, p0(image), rows0, rows[image])
    move.wait_recv()
    speeds(mine0, theirs0, 0, OWN, speed0)
    each(every, theta0)
    each(mids, next1)
    down[2].start()
    up[2].start()
    each(outs, drift0)
    each(mids, drift1)
    live_round(0)

    arrive(1)
    rows = {image: send_rows(phi0, p0(image), rows0) for image in (2, 9)}
    each(outs, gap0)
    move = exchange(mine0, theirs0, OWN, 2)
    for image in (2, 9):
        halo(phi0, p0(image), rows0, rows[image])
    move.wait_recv()
    speeds(mine0, theirs0, OWN, 2, speed0)
    each(outs, theta0)
    each(ends, next1)
    down[3].start()
    up[3].start()
    each(mids, gap1)
    move = exchange(mine1, theirs1, 0, 2)
    each(ends, drift1)
    move.wait_recv()
    speeds(mine1, theirs1, 0, 2, speed1)
    paces = [
        remote(speed1.at[0], speed1.at[7], pace_send.at[0], pace_recv.at[0], to_low),
        remote(speed1.at[1], speed1.at[6], pace_send.at[1], pace_recv.at[1], to_high),
    ]
    each(mids, theta1)
    for copy in paces + down[4:6] + up[4:6]:
        copy.start()
    live_round(1)

    arrive(2)
    rows = {image: send_rows(phi1, p1(image), rows1) for image in (2, 9)}
    each(outs, gap1)
    for image in (2, 9):
        halo(phi1, p1(image), rows1, rows[image])
    for image in (2, 9):
        drift(phi1, th1, p1(image), t1(image), slab)
    live_round(2)

    arrive(3)
    rows = {image: send_rows(phi1, p1(image), rows1) for image in (3, 8)}
    each(ends, gap1)
    move = exchange(mine1, theirs1, 2, 2)
    for image in (3, 8):
        halo(phi1, p1(image), rows1, rows[image])
    each(outs, drift1)
    last_move = exchange(mine1, theirs1, 4, 2)
    move.wait_recv()
    speeds(mine1, theirs1, 2, 2, speed1)
    each(ends, theta1)
    each(mids, next2)
    last_move.wait_recv()
    speeds(mine1, theirs1, 4, 2, speed1)
    each(outs, theta1)
    each(ends, next2)
    for image in (5, 6, 7):
        segment_sum(image, mine2.at[image - FIRST])
    live_round(3)

    for copy in paces:
        copy.wait_recv()
    arrive(4)

    def cross(low_tiles, high_tiles):
        theta1(2, low_tiles)
        theta1(9, high_tiles)
        next2(3, low_tiles)
        next2(8, high_tiles)

    cross(upper_half, lower_half)
    segment_sum(4, mine2.at[0], range(*upper_half))
    segment_sum(8, mine2.at[OWN], range(*lower_half))
    move = exchange(mine2, theirs2, 0, OWN + 1)
    move.wait_recv()

    lane = lax.broadcasted_iota(jnp.int32, (1, LANES), 1)
    squares = jnp.zeros((1, LANES), jnp.float32)
    for i in range(OWN + 1):
        squares = jnp.where(lane == i, whole(mine2[i] + theirs2[i])[0:1], squares)
    message[0] = squares
    gathered[img] = squares

    def send_length(k):
        return remote(message.at[0], gathered.at[img], len_send.at[k], len_recv.at[k], {"img": lax.rem(img + k, count)})

    def spread_out(i, carry):
        distance = count // 2 - 1 - i
        send_length(distance).start()
        send_length(count - distance).start()
        return carry

    send_length(count // 2).start()
    lax.fori_loop(0, count // 2 - 1, spread_out, 0)
    for group in down_new + [up_new]:
        for copy in group:
            copy.start()
    arrive(5)
    cross(lower_half, upper_half)

    def heard(k, carry):
        send_length(k).wait_recv()
        return carry

    lax.fori_loop(1, count, heard, 0)

    owner = lax.broadcasted_iota(jnp.int32, (count, 1, LANES), 0)
    spot = lax.broadcasted_iota(jnp.int32, (count, 1, LANES), 2)
    index = OWN * owner + spot
    squares = gathered[...]
    before = jnp.concatenate([squares[count - 1 :], squares[: count - 1]], axis=0)
    halves = jnp.where(spot == 0, squares, 0.0) + jnp.where(spot == OWN, before, 0.0)
    squares = jnp.where(spot == 0, jnp.sum(halves, axis=2, keepdims=True), squares)
    segs = jnp.where((spot < OWN) & (index > 0), jnp.sqrt(squares + EPSILON), 0.0)

    def add_up(a):
        return jnp.sum(jnp.sum(a, axis=0), axis=1, keepdims=True)

    length = add_up(segs)
    weights = []
    for i in range(OWN):
        base = bracket[i]
        arc = add_up(jnp.where(index <= base, segs, 0.0))
        seg = add_up(jnp.where(index == base + 1, segs, 0.0))
        target = length * (OWN * img + i).astype(jnp.float32) / jnp.float32(last)
        weights.append(jnp.broadcast_to((target - arc) / seg, (SUB, half)))

    writes = [pltpu.make_async_copy(result.at[t], out.at[t], out_sem.at[t]) for t in range(TILES)]
    for t in range(TILES):
        for group in down_new + [up_new]:
            group[t].wait_recv()
        for i in range(OWN):
            pick = jnp.clip(bracket[i] - (OWN * img - 2), 0, 7)
            for c in chunks:
                span = slice(c, c + half)
                base = phi2[t][pick, :, span]
                result[t, i, :, span] = base + weights[i] * (phi2[t][pick + 1, :, span] - base)
        writes[t].start()

    for copy in down + up + row_moves + swaps + paces + up_new + down_new[0] + down_new[1]:
        copy.wait_send()

    def sent(k, carry):
        send_length(k).wait_send()
        return carry

    lax.fori_loop(1, count, sent, 0)
    for copy in writes:
        copy.wait()


def per_device(count, path, bracket):
    images, rows, cols = path.shape
    f32 = jnp.float32
    dma = pltpu.SemaphoreType.DMA
    tiled = path.reshape(images, TILES, SUB, cols)

    def slabs(number, tiles=EXT):
        return pltpu.VMEM((number, tiles, SUB, cols), f32)

    def small(*dims):
        return pltpu.VMEM((*dims, SUB, LANES), f32)

    out = pl.pallas_call(
        functools.partial(kernel, count),
        out_shape=jax.ShapeDtypeStruct((TILES, images, SUB, cols), f32),
        in_specs=[pl.BlockSpec(memory_space=pl.ANY), pl.BlockSpec(memory_space=pltpu.SMEM)],
        out_specs=pl.BlockSpec(memory_space=pl.ANY),
        scratch_shapes=[
            slabs(8),
            slabs(10),
            *[pltpu.VMEM((9, SUB, cols), f32) for _ in range(TILES)],
            slabs(6),
            slabs(8),
            slabs(8, 2),
            slabs(10, 2),
            small(6, 2), small(6, 2),
            small(6, 2), small(6, 2),
            small(OWN + 1), small(OWN + 1),
            small(6), small(8),
            pltpu.VMEM((1, 1, LANES), f32),
            pltpu.VMEM((count, 1, LANES), f32),
            pltpu.VMEM((TILES, images, SUB, cols), f32),
            dma((OWN,)),
            dma((6,)), dma((6,)), dma((6,)), dma((6,)),
            dma((24,)), dma((24,)),
            dma((8,)), dma((8,)),
            dma((3, TILES)), dma((3, TILES)),
            dma((2,)), dma((2,)),
            dma((count,)), dma((count,)),
            dma((TILES,)),
            pltpu.SemaphoreType.REGULAR((8,)),
        ],
        compiler_params=pltpu.CompilerParams(
            collective_id=0, has_side_effects=True, vmem_limit_bytes=60 * 1024 * 1024
        ),
    )(tiled, bracket)
    return out.transpose(1, 0, 2, 3).reshape(images, rows, cols)


def solution(mesh):
    count = mesh.shape["img"]
    return jax.shard_map(
        functools.partial(per_device, count),
        mesh=mesh,
        in_specs=(P(("groups", "img"), "space", None), P(("groups", "img"))),
        out_specs=P(("groups", "img"), "space", None),
        check_vma=False,
    )
```

```python
import functools

import jax
import jax.numpy as jnp
from jax import lax
from jax.experimental import pallas as pl
from jax.experimental.pallas import tpu as pltpu
from jax.sharding import PartitionSpec as P

REACH = 2
ITERS = 2
TIME_STEP = 0.002
EPSILON = 1e-06

LANES = 128
SUB = 8
OWN = 4
TILES = 4
EXT = TILES + 1
FIRST = 4


def fold(block):
    parts = [block[:, i : i + LANES] for i in range(0, block.shape[1], LANES)]
    while len(parts) > 1:
        parts = [a + b for a, b in zip(parts[::2], parts[1::2])] + parts[len(parts) // 2 * 2 :]
    return parts[0]


def spread(vector, width):
    return jnp.concatenate([vector] * (width // LANES), axis=1)


def kernel(count, path, bracket, out, phi0, phi1, phi2_0, phi2_1, phi2_2, phi2_3, th0, th1, rows0, rows1,
           mine0, theirs0, mine1, theirs1, mine2, theirs2, speed0, speed1, message, gathered, result,
           local_sem, down_send, down_recv, up_send, up_recv, row_send, row_recv, sum_send, sum_recv,
           new_send, new_recv, pace_send, pace_recv, len_send, len_recv, out_sem, live):
    cols = path.shape[-1]
    half = min(cols, 1024)
    phi2 = (phi2_0, phi2_1, phi2_2, phi2_3)
    img = lax.axis_index("img")
    core = lax.axis_index("space")

    low = lax.rem(img + count - 1, count)
    high = lax.rem(img + 1, count)
    partner = 1 - core
    to_low, to_high, to_partner = {"img": low}, {"img": high}, {"space": partner}
    mesh_id = pl.DeviceIdType.MESH

    def remote(src, dst, send, recv, where):
        return pltpu.make_async_remote_copy(
            src_ref=src, dst_ref=dst, send_sem=send, recv_sem=recv, device_id=where, device_id_type=mesh_id
        )

    p0, p1, p2, t0, t1 = (lambda w, s=s: w - s for s in (2, 1, 2, 3, 2))

    loads = [
        pltpu.make_async_copy(path.at[i], phi0.at[p0(FIRST + i), pl.ds(0, TILES)], local_sem.at[i]) for i in range(OWN)
    ]
    for i in (0, 3, 1, 2):
        loads[i].start()

    barrier = pltpu.get_barrier_semaphore()
    def signal(sem, where):
        pl.semaphore_signal(sem, inc=1, device_id=where, device_id_type=mesh_id)

    has_low, has_high = img > 0, img < count - 1
    pl.when(has_low)(lambda: signal(barrier, to_low))
    pl.when(has_high)(lambda: signal(barrier, to_high))
    signal(barrier, to_partner)
    pl.semaphore_wait(barrier, 1 + has_low.astype(jnp.int32) + has_high.astype(jnp.int32))

    def when(condition, copies, act):
        @pl.when(condition)
        def _():
            for copy in copies:
                getattr(copy, act)()

    def part(ref, slot, first=0, number=TILES):
        return ref.at[slot, pl.ds(first, number)]

    def shift(ref, name, source, target, k, where, first=0, number=TILES):
        send, recv = (down_send, down_recv) if where is to_low else (up_send, up_recv)
        return remote(part(ref, name(source), first, number), part(ref, name(target), first, number),
                      send.at[k], recv.at[k], where)

    down = [
        shift(phi0, p0, 4, 8, 0, to_low), shift(phi0, p0, 5, 9, 1, to_low),
        shift(phi1, p1, 5, 9, 2, to_low), shift(phi1, p1, 4, 8, 3, to_low),
        shift(phi1, p1, 6, 10, 4, to_low, 2, 2), shift(phi1, p1, 6, 10, 5, to_low, 0, 2),
    ]
    up = [
        shift(phi0, p0, 7, 3, 0, to_high), shift(phi0, p0, 6, 2, 1, to_high),
        shift(phi1, p1, 6, 2, 2, to_high), shift(phi1, p1, 7, 3, 3, to_high),
        shift(phi1, p1, 5, 1, 4, to_high, 0, 2), shift(phi1, p1, 5, 1, 5, to_high, 2, 2),
    ]
    down_new = [
        [remote(phi2[t].at[p2(source)], phi2[t].at[p2(target)], new_send.at[k, t], new_recv.at[k, t], to_low)
         for t in range(TILES)]
        for k, (source, target) in enumerate(((5, 9), (6, 10)))
    ]
    up_new = [
        remote(phi2[t].at[p2(6)], phi2[t].at[p2(2)], new_send.at[2, t], new_recv.at[2, t], to_high)
        for t in range(TILES)
    ]

    def go_down(*copies):
        when(has_low, copies, "start")

    def go_up(*copies):
        when(has_high, copies, "start")

    row_moves = []

    def send_rows(ref, slot, rows):
        copies = []
        for k, tile in enumerate((0, TILES - 1)):
            n = len(row_moves)
            copy = remote(ref.at[slot, tile], rows.at[slot, k], row_send.at[n], row_recv.at[n], to_partner)
            copy.start()
            row_moves.append(copy)
            copies.append(copy)
        return copies

    def halo(ref, slot, rows, copies):
        for copy in copies:
            copy.wait_recv()
        for c in chunks:
            ref[slot, TILES, :, c : c + half] = jnp.where(
                sub < SUB // 2, rows[slot, 0, :, c : c + half], rows[slot, 1, :, c : c + half]
            )

    sub = lax.broadcasted_iota(jnp.int32, (SUB, half), 0)
    chunks = range(0, cols, half)

    for i in (0, 3, 1, 2):
        loads[i].wait()
        if i < 2:
            go_down(down[i])
        else:
            go_up(up[3 - i])
    own_rows = [send_rows(phi0, p0(image), rows0) for image in range(FIRST, FIRST + OWN)]
    lives = []
    while 2 ** len(lives) < count - 1:
        lives.append(2 ** len(lives))

    def say_live(n):
        for where in (img - lives[n], img + lives[n]):
            pl.when((where >= 0) & (where < count))(lambda where=where: signal(live.at[n], {"img": where}))

    def hear_live(n):
        below, above = img >= lives[n], img < count - lives[n]
        pl.semaphore_wait(live.at[n], below.astype(jnp.int32) + above.astype(jnp.int32))

    if lives:
        say_live(0)

    is_first = (img == 0).astype(jnp.int32)
    is_last = (img == count - 1).astype(jnp.int32)
    last = OWN * count - 1

    def same(image, k):
        return jnp.asarray(image == k).astype(jnp.int32)

    def sides(image):
        at_first = is_first * same(image, FIRST)
        at_last = is_last * same(image, FIRST + OWN - 1)
        end = (at_first + at_last).astype(jnp.float32)
        return image - 1 + at_first, image + 1 - at_last, (1.0 + end) * jnp.float32(last / 2.0)

    def around(ref, slot, tile, c):
        above = lax.rem(tile + EXT - 1, EXT)
        below = lax.rem(tile + 1, EXT)
        here = ref[slot, tile, :, c : c + half]
        up_rows = pltpu.roll(jnp.where(sub == SUB - 1, ref[slot, above, :, c : c + half], here), 1, 0)
        down_rows = pltpu.roll(jnp.where(sub == 0, ref[slot, below, :, c : c + half], here), SUB - 1, 0)
        if half == cols:
            left = pltpu.roll(here, 1, 1)
            right = pltpu.roll(here, half - 1, 1)
        else:
            before = (c - LANES) % cols
            after = (c + half) % cols
            wide = jnp.concatenate(
                [ref[slot, tile, :, before : before + LANES], here, ref[slot, tile, :, after : after + LANES]], axis=1
            )
            left = pltpu.roll(wide, 1, 1)[:, LANES : LANES + half]
            right = pltpu.roll(wide, half + 2 * LANES - 1, 1)[:, LANES : LANES + half]
        return here, (up_rows + down_rows) + (left + right) - 4.0 * here

    zero = jnp.zeros((SUB, LANES), jnp.float32)

    def over(tiles, one, init):
        first, end = tiles
        return lax.fori_loop(first, end, one, init)

    full, slab, upper_half, lower_half = (0, EXT), (0, TILES), (0, 2), (2, TILES)

    def drift(phi, th, slot, th_slot, tiles, total=None):
        def one(tile, acc):
            for c in chunks:
                here, lap = around(phi, slot, tile, c)
                force = lap + here - here * here * here
                th[th_slot, tile, :, c : c + half] = force
                acc = acc + jnp.where(tile < TILES, fold(force * force), 0.0)
            return acc

        acc = over(tiles, one, zero)
        if total is not None:
            total[...] = acc

    def stretch_sum(phi, lower, upper, total, factor):
        def one(tile, acc):
            for c in chunks:
                gap = phi[upper, tile, :, c : c + half] - phi[lower, tile, :, c : c + half]
                acc = acc + fold(gap * gap)
            return acc

        total[...] = over(slab, one, zero) * (factor * factor)

    def segment_sum(image, total, tiles=range(TILES)):
        acc = zero
        for t in tiles:
            for c in chunks:
                gap = phi2[t][p2(image), :, c : c + half] - phi2[t][p2(image - 1), :, c : c + half]
                acc = acc + fold(gap * gap)
        total[...] = acc

    def theta(phi, th, lower, upper, factor, th_slot, speed, tiles):
        scale = spread(speed * factor, half)

        def one(tile, carry):
            for c in chunks:
                span = slice(c, c + half)
                gap = phi[upper, tile, :, span] - phi[lower, tile, :, span]
                th[th_slot, tile, :, span] = scale * gap - th[th_slot, tile, :, span]
            return carry

        over(tiles, one, 0)

    def advance(phi, slot, th, th_slot, new, new_slot, speed, image, tiles):
        fixed = is_first * same(image, FIRST) + is_last * same(image, FIRST + OWN - 1)
        scale = spread(speed * jnp.float32(last / 2.0), half)

        def one(tile, carry):
            for c in chunks:
                span = slice(c, c + half)
                here, lap = around(th, th_slot, tile, c)
                old = phi[slot, tile, :, span]
                bend = th[th_slot + 1, tile, :, span] - th[th_slot - 1, tile, :, span]
                descent = scale * bend + lap + (1.0 - 3.0 * old * old) * here
                value = jnp.where(fixed == 0, old + TIME_STEP * descent, old)
                if new is phi2:
                    new[tile][new_slot, :, span] = value
                else:
                    new[new_slot, tile, :, span] = value
            return carry

        if new is phi2:
            for tile in range(*tiles):
                one(tile, 0)
        else:
            over(tiles, one, 0)

    def whole(a):
        return jnp.broadcast_to(jnp.sum(jnp.sum(a, axis=1, keepdims=True), axis=0, keepdims=True), (SUB, LANES))

    def speeds(mine, theirs, first, number, out_ref):
        for i in range(first, first + number):
            force = whole(mine[i, 0] + theirs[i, 0])
            stretch = whole(mine[i, 1] + theirs[i, 1])
            out_ref[i] = jnp.sqrt(force + EPSILON) / jnp.sqrt(stretch + EPSILON)

    def place(image):
        if isinstance(image, int):
            return 2 * (5 - image) if image < 6 else 2 * (image - 6) + 1
        return jnp.where(image < 6, 2 * (5 - image), 2 * (image - 6) + 1)

    def each(images, body):
        start, step, number = images

        def one(i, carry):
            body(start + step * i)
            return carry

        lax.fori_loop(0, number, one, 0)

    every, mids, ends, outs = (4, 1, 4), (5, 1, 2), (4, 3, 2), (3, 5, 2)

    def gap0(image):
        lower, upper, factor = sides(image)
        stretch_sum(phi0, p0(lower), p0(upper), mine0.at[place(image), 1], factor)

    def drift0(image):
        drift(phi0, th0, p0(image), t0(image), full, mine0.at[place(image), 0])

    def theta0(image):
        lower, upper, factor = sides(image)
        theta(phi0, th0, p0(lower), p0(upper), factor, t0(image), speed0[place(image)], full)

    def next1(image):
        advance(phi0, p0(image), th0, t0(image), phi1, p1(image), speed0[place(image)], image, full)

    def gap1(image):
        lower, upper, factor = sides(image)
        stretch_sum(phi1, p1(lower), p1(upper), mine1.at[place(image), 1], factor)

    def drift1(image):
        drift(phi1, th1, p1(image), t1(image), full, mine1.at[place(image), 0])

    def theta1(image, tiles=full):
        lower, upper, factor = sides(image)
        theta(phi1, th1, p1(lower), p1(upper), factor, t1(image), speed1[place(image)], tiles)

    def next2(image, tiles=slab):
        advance(phi1, p1(image), th1, t1(image), phi2, p2(image), speed1[place(image)], image, tiles)

    swaps = []

    def exchange(mine, theirs, first, number):
        k = len(swaps)
        span = pl.ds(first, number)
        move = remote(mine.at[span], theirs.at[span], sum_send.at[k], sum_recv.at[k], to_partner)
        move.start()
        swaps.append(move)
        return move

    def arrive(k):
        when(has_high, [down[k]], "wait_recv")
        when(has_low, [up[k]], "wait_recv")

    def live_round(n):
        if n < len(lives):
            hear_live(n)
            if n + 1 < len(lives):
                say_live(n + 1)

    for image in range(FIRST, FIRST + OWN):
        halo(phi0, p0(image), rows0, own_rows[image - FIRST])
    live_round(0)
    each(every, drift0)
    each(mids, gap0)
    live_round(1)

    arrive(0)
    rows = {image: send_rows(phi0, p0(image), rows0) for image in (3, 8)}
    each(ends, gap0)
    move = exchange(mine0, theirs0, 0, OWN)
    for image in (3, 8):
        halo(phi0, p0(image), rows0, rows[image])
    move.wait_recv()
    speeds(mine0, theirs0, 0, OWN, speed0)
    each(every, theta0)
    each(mids, next1)
    go_down(down[2])
    go_up(up[2])
    each(outs, drift0)
    each(mids, drift1)
    live_round(2)

    arrive(1)
    rows = {image: send_rows(phi0, p0(image), rows0) for image in (2, 9)}
    each(outs, gap0)
    move = exchange(mine0, theirs0, OWN, 2)
    for image in (2, 9):
        halo(phi0, p0(image), rows0, rows[image])
    move.wait_recv()
    speeds(mine0, theirs0, OWN, 2, speed0)
    each(outs, theta0)
    each(ends, next1)
    go_down(down[3])
    go_up(up[3])
    each(mids, gap1)
    move = exchange(mine1, theirs1, 0, 2)
    each(ends, drift1)
    move.wait_recv()
    speeds(mine1, theirs1, 0, 2, speed1)
    paces = [
        remote(speed1.at[0], speed1.at[7], pace_send.at[0], pace_recv.at[0], to_low),
        remote(speed1.at[1], speed1.at[6], pace_send.at[1], pace_recv.at[1], to_high),
    ]
    each(mids, theta1)
    go_down(paces[0], *down[4:6])
    go_up(paces[1], *up[4:6])
    live_round(3)

    arrive(2)
    rows = {image: send_rows(phi1, p1(image), rows1) for image in (2, 9)}
    each(outs, gap1)
    for image in (2, 9):
        halo(phi1, p1(image), rows1, rows[image])
    for image in (2, 9):
        drift(phi1, th1, p1(image), t1(image), slab)

    arrive(3)
    rows = {image: send_rows(phi1, p1(image), rows1) for image in (3, 8)}
    each(ends, gap1)
    move = exchange(mine1, theirs1, 2, 2)
    for image in (3, 8):
        halo(phi1, p1(image), rows1, rows[image])
    each(outs, drift1)
    last_move = exchange(mine1, theirs1, 4, 2)
    move.wait_recv()
    speeds(mine1, theirs1, 2, 2, speed1)
    each(ends, theta1)
    each(mids, next2)
    last_move.wait_recv()
    speeds(mine1, theirs1, 4, 2, speed1)
    each(outs, theta1)
    each(ends, next2)
    for image in (5, 6, 7):
        segment_sum(image, mine2.at[image - FIRST])

    when(has_high, [paces[0]], "wait_recv")
    when(has_low, [paces[1]], "wait_recv")
    arrive(4)

    def cross(low_tiles, high_tiles):
        theta1(2, low_tiles)
        theta1(9, high_tiles)
        next2(3, low_tiles)
        next2(8, high_tiles)

    cross(upper_half, lower_half)
    segment_sum(4, mine2.at[0], range(*upper_half))
    segment_sum(8, mine2.at[OWN], range(*lower_half))
    move = exchange(mine2, theirs2, 0, OWN + 1)
    move.wait_recv()

    lane = lax.broadcasted_iota(jnp.int32, (1, LANES), 1)
    squares = jnp.zeros((1, LANES), jnp.float32)
    for i in range(OWN + 1):
        squares = jnp.where(lane == i, whole(mine2[i] + theirs2[i])[0:1], squares)
    message[0] = squares
    gathered[img] = squares

    live_round(4)

    def send_length(k):
        return remote(message.at[0], gathered.at[img], len_send.at[k], len_recv.at[k], {"img": lax.rem(img + k, count)})

    def spread_out(i, carry):
        distance = count // 2 - 1 - i
        send_length(distance).start()
        send_length(count - distance).start()
        return carry

    send_length(count // 2).start()
    lax.fori_loop(0, count // 2 - 1, spread_out, 0)
    go_down(*down_new[0], *down_new[1])
    go_up(*up_new)
    arrive(5)
    cross(lower_half, upper_half)

    def heard(k, carry):
        send_length(k).wait_recv()
        return carry

    lax.fori_loop(1, count, heard, 0)

    owner = lax.broadcasted_iota(jnp.int32, (count, 1, LANES), 0)
    spot = lax.broadcasted_iota(jnp.int32, (count, 1, LANES), 2)
    index = OWN * owner + spot
    squares = gathered[...]
    before = jnp.concatenate([squares[count - 1 :], squares[: count - 1]], axis=0)
    halves = jnp.where(spot == 0, squares, 0.0) + jnp.where(spot == OWN, before, 0.0)
    squares = jnp.where(spot == 0, jnp.sum(halves, axis=2, keepdims=True), squares)
    segs = jnp.where((spot < OWN) & (index > 0), jnp.sqrt(squares + EPSILON), 0.0)

    def add_up(a):
        return jnp.sum(jnp.sum(a, axis=0), axis=1, keepdims=True)

    length = add_up(segs)
    weights = []
    for i in range(OWN):
        base = bracket[i]
        arc = add_up(jnp.where(index <= base, segs, 0.0))
        seg = add_up(jnp.where(index == base + 1, segs, 0.0))
        target = length * (OWN * img + i).astype(jnp.float32) / jnp.float32(last)
        weights.append(jnp.broadcast_to((target - arc) / seg, (SUB, half)))

    writes = [pltpu.make_async_copy(result.at[t], out.at[pl.ds(0, OWN), t], out_sem.at[t]) for t in range(TILES)]
    for t in range(TILES):
        when(has_high, [down_new[0][t], down_new[1][t]], "wait_recv")
        when(has_low, [up_new[t]], "wait_recv")
        for i in range(OWN):
            pick = jnp.clip(bracket[i] - (OWN * img - 2), 0, 7)
            for c in chunks:
                span = slice(c, c + half)
                base = phi2[t][pick, :, span]
                result[t, i, :, span] = base + weights[i] * (phi2[t][pick + 1, :, span] - base)
        writes[t].start()

    when(has_low, down + down_new[0] + down_new[1] + paces[:1], "wait_send")
    when(has_high, up + up_new + paces[1:], "wait_send")
    for copy in row_moves + swaps:
        copy.wait_send()

    def sent(k, carry):
        send_length(k).wait_send()
        return carry

    lax.fori_loop(1, count, sent, 0)
    for copy in writes:
        copy.wait()


def per_device(count, path, bracket):
    images, rows, cols = path.shape
    f32 = jnp.float32
    dma = pltpu.SemaphoreType.DMA
    tiled = path.reshape(images, TILES, SUB, cols)

    def slabs(number, tiles=EXT):
        return pltpu.VMEM((number, tiles, SUB, cols), f32)

    def small(*dims):
        return pltpu.VMEM((*dims, SUB, LANES), f32)

    out = pl.pallas_call(
        functools.partial(kernel, count),
        out_shape=jax.ShapeDtypeStruct((images, TILES, SUB, cols), f32),
        in_specs=[pl.BlockSpec(memory_space=pl.ANY), pl.BlockSpec(memory_space=pltpu.SMEM)],
        out_specs=pl.BlockSpec(memory_space=pl.ANY),
        scratch_shapes=[
            slabs(8),
            slabs(10),
            *[pltpu.VMEM((9, SUB, cols), f32) for _ in range(TILES)],
            slabs(6),
            slabs(8),
            slabs(8, 2),
            slabs(10, 2),
            small(6, 2), small(6, 2),
            small(6, 2), small(6, 2),
            small(OWN + 1), small(OWN + 1),
            small(6), small(8),
            pltpu.VMEM((1, 1, LANES), f32),
            pltpu.VMEM((count, 1, LANES), f32),
            pltpu.VMEM((TILES, images, SUB, cols), f32),
            dma((OWN,)),
            dma((6,)), dma((6,)), dma((6,)), dma((6,)),
            dma((24,)), dma((24,)),
            dma((8,)), dma((8,)),
            dma((3, TILES)), dma((3, TILES)),
            dma((2,)), dma((2,)),
            dma((count,)), dma((count,)),
            dma((TILES,)),
            pltpu.SemaphoreType.REGULAR((8,)),
        ],
        compiler_params=pltpu.CompilerParams(
            collective_id=0, has_side_effects=True, vmem_limit_bytes=60 * 1024 * 1024
        ),
    )(tiled, bracket)
    return out.reshape(images, rows, cols)


def solution(mesh):
    count = mesh.shape["img"]
    return jax.shard_map(
        functools.partial(per_device, count),
        mesh=mesh,
        in_specs=(P(("groups", "img"), "space", None), P(("groups", "img"))),
        out_specs=P(("groups", "img"), "space", None),
        check_vma=False,
    )
```

```python
import functools

import jax
import jax.numpy as jnp
from jax import lax
from jax.experimental import pallas as pl
from jax.experimental.pallas import tpu as pltpu
from jax.sharding import PartitionSpec as P

REACH = 2
ITERS = 2
TIME_STEP = 0.002
EPSILON = 1e-06

LANES = 128
SUB = 8
OWN = 4
TILES = 4
EXT = TILES + 1
FIRST = 4


def fold(block):
    parts = [block[:, i : i + LANES] for i in range(0, block.shape[1], LANES)]
    while len(parts) > 1:
        parts = [a + b for a, b in zip(parts[::2], parts[1::2])] + parts[len(parts) // 2 * 2 :]
    return parts[0]


def spread(vector, width):
    return jnp.concatenate([vector] * (width // LANES), axis=1)


def kernel(count, path, given, out, phi0, phi1, phi2_0, phi2_1, phi2_2, phi2_3, th0, th1, rows0, rows1,
           mine0, theirs0, mine1, theirs1, mine2, theirs2, speed0, speed1, message, gathered, lengths,
           local_sem, down_send, down_recv, up_send, up_recv, row_send, row_recv, sum_send, sum_recv,
           new_send, new_recv, pace_send, pace_recv, len_send, len_recv, bracket, given_sem, live):
    cols = path.shape[-1]
    half = min(cols, 1024)
    phi2 = (phi2_0, phi2_1, phi2_2, phi2_3)
    img = lax.axis_index("img")
    core = lax.axis_index("space")

    low = lax.rem(img + count - 1, count)
    high = lax.rem(img + 1, count)
    partner = 1 - core
    to_low, to_high, to_partner = {"img": low}, {"img": high}, {"space": partner}
    mesh_id = pl.DeviceIdType.MESH

    def remote(src, dst, send, recv, where):
        return pltpu.make_async_remote_copy(
            src_ref=src, dst_ref=dst, send_sem=send, recv_sem=recv, device_id=where, device_id_type=mesh_id
        )

    p0, p1, p2, t0, t1 = (lambda w, s=s: w - s for s in (2, 1, 2, 3, 2))

    loads = [
        pltpu.make_async_copy(path.at[i], phi0.at[p0(FIRST + i), pl.ds(0, TILES)], local_sem.at[i]) for i in range(OWN)
    ]
    for i in (0, 3, 1, 2):
        loads[i].start()
    given_load = pltpu.make_async_copy(given, bracket, given_sem)
    given_load.start()

    barrier = pltpu.get_barrier_semaphore()
    def signal(sem, where):
        pl.semaphore_signal(sem, inc=1, device_id=where, device_id_type=mesh_id)

    has_low, has_high = img > 0, img < count - 1
    pl.when(has_low)(lambda: signal(barrier, to_low))
    pl.when(has_high)(lambda: signal(barrier, to_high))
    neighbours = has_low.astype(jnp.int32) + has_high.astype(jnp.int32)
    pl.semaphore_wait(barrier, neighbours + (1 - core))
    signal(barrier, to_partner)

    def when(condition, copies, act):
        @pl.when(condition)
        def _():
            for copy in copies:
                getattr(copy, act)()

    def part(ref, slot, first=0, number=TILES):
        return ref.at[slot, pl.ds(first, number)]

    def shift(ref, name, source, target, k, where, first=0, number=TILES):
        send, recv = (down_send, down_recv) if where is to_low else (up_send, up_recv)
        return remote(part(ref, name(source), first, number), part(ref, name(target), first, number),
                      send.at[k], recv.at[k], where)

    down = [
        shift(phi0, p0, 4, 8, 0, to_low), shift(phi0, p0, 5, 9, 1, to_low),
        shift(phi1, p1, 5, 9, 2, to_low), shift(phi1, p1, 4, 8, 3, to_low),
        shift(phi1, p1, 6, 10, 4, to_low, 2, 2), shift(phi1, p1, 6, 10, 5, to_low, 0, 2),
    ]
    up = [
        shift(phi0, p0, 7, 3, 0, to_high), shift(phi0, p0, 6, 2, 1, to_high),
        shift(phi1, p1, 6, 2, 2, to_high), shift(phi1, p1, 7, 3, 3, to_high),
        shift(phi1, p1, 5, 1, 4, to_high, 0, 2), shift(phi1, p1, 5, 1, 5, to_high, 2, 2),
    ]
    down_new = [
        [remote(phi2[t].at[p2(source)], phi2[t].at[p2(target)], new_send.at[k, t], new_recv.at[k, t], to_low)
         for t in range(TILES)]
        for k, (source, target) in enumerate(((5, 9), (6, 10)))
    ]
    up_new = [
        remote(phi2[t].at[p2(6)], phi2[t].at[p2(2)], new_send.at[2, t], new_recv.at[2, t], to_high)
        for t in range(TILES)
    ]

    def go_down(*copies):
        when(has_low, copies, "start")

    def go_up(*copies):
        when(has_high, copies, "start")

    row_moves = []

    def send_rows(ref, slot, rows):
        copies = []
        for k, tile in enumerate((0, TILES - 1)):
            n = len(row_moves)
            copy = remote(ref.at[slot, tile], rows.at[slot, k], row_send.at[n], row_recv.at[n], to_partner)
            copy.start()
            row_moves.append(copy)
            copies.append(copy)
        return copies

    def halo(ref, slot, rows, copies):
        for copy in copies:
            copy.wait_recv()
        for c in chunks:
            ref[slot, TILES, :, c : c + half] = jnp.where(
                sub < SUB // 2, rows[slot, 0, :, c : c + half], rows[slot, 1, :, c : c + half]
            )

    sub = lax.broadcasted_iota(jnp.int32, (SUB, half), 0)
    chunks = range(0, cols, half)

    for i in (0, 3, 1, 2):
        loads[i].wait()
        if i < 2:
            go_down(down[i])
        else:
            go_up(up[3 - i])
    pl.when(core == 1)(lambda: pl.semaphore_wait(barrier, 1))
    own_rows = [send_rows(phi0, p0(image), rows0) for image in range(FIRST, FIRST + OWN)]
    lives = []
    while 2 ** len(lives) < count - 1:
        lives.append(2 ** len(lives))

    def say_live(n):
        for where in (img - lives[n], img + lives[n]):
            pl.when((where >= 0) & (where < count))(lambda where=where: signal(live.at[n], {"img": where}))

    def hear_live(n):
        below, above = img >= lives[n], img < count - lives[n]
        pl.semaphore_wait(live.at[n], below.astype(jnp.int32) + above.astype(jnp.int32))

    if lives:
        say_live(0)

    is_first = (img == 0).astype(jnp.int32)
    is_last = (img == count - 1).astype(jnp.int32)
    last = OWN * count - 1

    def same(image, k):
        return jnp.asarray(image == k).astype(jnp.int32)

    def sides(image):
        at_first = is_first * same(image, FIRST)
        at_last = is_last * same(image, FIRST + OWN - 1)
        end = (at_first + at_last).astype(jnp.float32)
        return image - 1 + at_first, image + 1 - at_last, (1.0 + end) * jnp.float32(last / 2.0)

    def around(ref, slot, tile, c):
        above = lax.rem(tile + EXT - 1, EXT)
        below = lax.rem(tile + 1, EXT)
        here = ref[slot, tile, :, c : c + half]
        up_rows = pltpu.roll(jnp.where(sub == SUB - 1, ref[slot, above, :, c : c + half], here), 1, 0)
        down_rows = pltpu.roll(jnp.where(sub == 0, ref[slot, below, :, c : c + half], here), SUB - 1, 0)
        if half == cols:
            left = pltpu.roll(here, 1, 1)
            right = pltpu.roll(here, half - 1, 1)
        else:
            before = (c - LANES) % cols
            after = (c + half) % cols
            wide = jnp.concatenate(
                [ref[slot, tile, :, before : before + LANES], here, ref[slot, tile, :, after : after + LANES]], axis=1
            )
            left = pltpu.roll(wide, 1, 1)[:, LANES : LANES + half]
            right = pltpu.roll(wide, half + 2 * LANES - 1, 1)[:, LANES : LANES + half]
        return here, (up_rows + down_rows) + (left + right) - 4.0 * here

    zero = jnp.zeros((SUB, LANES), jnp.float32)

    def over(tiles, one, init):
        first, end = tiles
        return lax.fori_loop(first, end, one, init)

    full, slab, upper_half, lower_half = (0, EXT), (0, TILES), (0, 2), (2, TILES)

    def drift(phi, th, slot, th_slot, tiles, total=None):
        def one(tile, acc):
            for c in chunks:
                here, lap = around(phi, slot, tile, c)
                force = lap + here - here * here * here
                th[th_slot, tile, :, c : c + half] = force
                acc = acc + jnp.where(tile < TILES, fold(force * force), 0.0)
            return acc

        acc = over(tiles, one, zero)
        if total is not None:
            total[...] = acc

    def stretch_sum(phi, lower, upper, total, factor):
        def one(tile, acc):
            for c in chunks:
                gap = phi[upper, tile, :, c : c + half] - phi[lower, tile, :, c : c + half]
                acc = acc + fold(gap * gap)
            return acc

        total[...] = over(slab, one, zero) * (factor * factor)

    def segment_sum(image, total, tiles=range(TILES)):
        acc = zero
        for t in tiles:
            for c in chunks:
                gap = phi2[t][p2(image), :, c : c + half] - phi2[t][p2(image - 1), :, c : c + half]
                acc = acc + fold(gap * gap)
        total[...] = acc

    def theta(phi, th, lower, upper, factor, th_slot, speed, tiles):
        scale = spread(speed * factor, half)

        def one(tile, carry):
            for c in chunks:
                span = slice(c, c + half)
                gap = phi[upper, tile, :, span] - phi[lower, tile, :, span]
                th[th_slot, tile, :, span] = scale * gap - th[th_slot, tile, :, span]
            return carry

        over(tiles, one, 0)

    def advance(phi, slot, th, th_slot, new, new_slot, speed, image, tiles):
        fixed = is_first * same(image, FIRST) + is_last * same(image, FIRST + OWN - 1)
        scale = spread(speed * jnp.float32(last / 2.0), half)

        def one(tile, carry):
            for c in chunks:
                span = slice(c, c + half)
                here, lap = around(th, th_slot, tile, c)
                old = phi[slot, tile, :, span]
                bend = th[th_slot + 1, tile, :, span] - th[th_slot - 1, tile, :, span]
                descent = scale * bend + lap + (1.0 - 3.0 * old * old) * here
                value = jnp.where(fixed == 0, old + TIME_STEP * descent, old)
                if new is phi2:
                    new[tile][new_slot, :, span] = value
                else:
                    new[new_slot, tile, :, span] = value
            return carry

        if new is phi2:
            for tile in range(*tiles):
                one(tile, 0)
        else:
            over(tiles, one, 0)

    def whole(a):
        return jnp.broadcast_to(jnp.sum(jnp.sum(a, axis=1, keepdims=True), axis=0, keepdims=True), (SUB, LANES))

    def speeds(mine, theirs, first, number, out_ref):
        for i in range(first, first + number):
            force = whole(mine[i, 0] + theirs[i, 0])
            stretch = whole(mine[i, 1] + theirs[i, 1])
            out_ref[i] = jnp.sqrt(force + EPSILON) / jnp.sqrt(stretch + EPSILON)

    def place(image):
        if isinstance(image, int):
            return 2 * (5 - image) if image < 6 else 2 * (image - 6) + 1
        return jnp.where(image < 6, 2 * (5 - image), 2 * (image - 6) + 1)

    def each(images, body):
        start, step, number = images

        def one(i, carry):
            body(start + step * i)
            return carry

        lax.fori_loop(0, number, one, 0)

    every, mids, ends, outs = (4, 1, 4), (5, 1, 2), (4, 3, 2), (3, 5, 2)

    def gap0(image):
        lower, upper, factor = sides(image)
        stretch_sum(phi0, p0(lower), p0(upper), mine0.at[place(image), 1], factor)

    def drift0(image):
        drift(phi0, th0, p0(image), t0(image), full, mine0.at[place(image), 0])

    def theta0(image):
        lower, upper, factor = sides(image)
        theta(phi0, th0, p0(lower), p0(upper), factor, t0(image), speed0[place(image)], full)

    def next1(image):
        advance(phi0, p0(image), th0, t0(image), phi1, p1(image), speed0[place(image)], image, full)

    def gap1(image):
        lower, upper, factor = sides(image)
        stretch_sum(phi1, p1(lower), p1(upper), mine1.at[place(image), 1], factor)

    def drift1(image):
        drift(phi1, th1, p1(image), t1(image), full, mine1.at[place(image), 0])

    def theta1(image, tiles=full):
        lower, upper, factor = sides(image)
        theta(phi1, th1, p1(lower), p1(upper), factor, t1(image), speed1[place(image)], tiles)

    def next2(image, tiles=slab):
        advance(phi1, p1(image), th1, t1(image), phi2, p2(image), speed1[place(image)], image, tiles)

    swaps = []

    def exchange(mine, theirs, first, number):
        k = len(swaps)
        span = pl.ds(first, number)
        move = remote(mine.at[span], theirs.at[span], sum_send.at[k], sum_recv.at[k], to_partner)
        move.start()
        swaps.append(move)
        return move

    def arrive(k):
        when(has_high, [down[k]], "wait_recv")
        when(has_low, [up[k]], "wait_recv")

    def live_round(n):
        if n < len(lives):
            hear_live(n)
            if n + 1 < len(lives):
                say_live(n + 1)

    for image in range(FIRST, FIRST + OWN):
        halo(phi0, p0(image), rows0, own_rows[image - FIRST])
    live_round(0)
    each(every, drift0)
    each(mids, gap0)
    live_round(1)

    arrive(0)
    rows = {image: send_rows(phi0, p0(image), rows0) for image in (3, 8)}
    each(ends, gap0)
    move = exchange(mine0, theirs0, 0, OWN)
    for image in (3, 8):
        halo(phi0, p0(image), rows0, rows[image])
    move.wait_recv()
    speeds(mine0, theirs0, 0, OWN, speed0)
    each(every, theta0)
    each(mids, next1)
    go_down(down[2])
    go_up(up[2])
    each(outs, drift0)
    each(mids, drift1)
    live_round(2)

    arrive(1)
    rows = {image: send_rows(phi0, p0(image), rows0) for image in (2, 9)}
    each(outs, gap0)
    move = exchange(mine0, theirs0, OWN, 2)
    for image in (2, 9):
        halo(phi0, p0(image), rows0, rows[image])
    move.wait_recv()
    speeds(mine0, theirs0, OWN, 2, speed0)
    each(outs, theta0)
    each(ends, next1)
    go_down(down[3])
    go_up(up[3])
    each(mids, gap1)
    move = exchange(mine1, theirs1, 0, 2)
    each(ends, drift1)
    move.wait_recv()
    speeds(mine1, theirs1, 0, 2, speed1)
    paces = [
        remote(speed1.at[0], speed1.at[7], pace_send.at[0], pace_recv.at[0], to_low),
        remote(speed1.at[1], speed1.at[6], pace_send.at[1], pace_recv.at[1], to_high),
    ]
    each(mids, theta1)
    go_down(paces[0], *down[4:6])
    go_up(paces[1], *up[4:6])
    live_round(3)

    arrive(2)
    rows = {image: send_rows(phi1, p1(image), rows1) for image in (2, 9)}
    each(outs, gap1)
    for image in (2, 9):
        halo(phi1, p1(image), rows1, rows[image])
    for image in (2, 9):
        drift(phi1, th1, p1(image), t1(image), slab)

    arrive(3)
    rows = {image: send_rows(phi1, p1(image), rows1) for image in (3, 8)}
    each(ends, gap1)
    move = exchange(mine1, theirs1, 2, 2)
    for image in (3, 8):
        halo(phi1, p1(image), rows1, rows[image])
    each(outs, drift1)
    last_move = exchange(mine1, theirs1, 4, 2)
    move.wait_recv()
    speeds(mine1, theirs1, 2, 2, speed1)
    each(ends, theta1)
    each(mids, next2)
    last_move.wait_recv()
    speeds(mine1, theirs1, 4, 2, speed1)
    each(outs, theta1)
    each(ends, next2)
    for image in (5, 6, 7):
        segment_sum(image, mine2.at[image - FIRST])

    when(has_high, [paces[0]], "wait_recv")
    when(has_low, [paces[1]], "wait_recv")
    arrive(4)

    def cross(low_tiles, high_tiles):
        theta1(2, low_tiles)
        theta1(9, high_tiles)
        next2(3, low_tiles)
        next2(8, high_tiles)

    cross(upper_half, lower_half)
    segment_sum(4, mine2.at[0], range(*upper_half))
    segment_sum(8, mine2.at[OWN], range(*lower_half))
    move = exchange(mine2, theirs2, 0, OWN + 1)
    move.wait_recv()

    lane = lax.broadcasted_iota(jnp.int32, (1, LANES), 1)
    squares = jnp.zeros((1, LANES), jnp.float32)
    for i in range(OWN + 1):
        squares = jnp.where(lane == i, whole(mine2[i] + theirs2[i])[0:1], squares)
    message[0] = squares
    gathered[img] = squares

    live_round(4)

    def send_length(k):
        return remote(message.at[0], gathered.at[img], len_send.at[k], len_recv.at[k], {"img": lax.rem(img + k, count)})

    def spread_out(i, carry):
        distance = count // 2 - 1 - i
        send_length(distance).start()
        send_length(count - distance).start()
        return carry

    @pl.when(core == 1)
    def _():
        send_length(count // 2).start()
        lax.fori_loop(0, count // 2 - 1, spread_out, 0)

    go_down(*down_new[0], *down_new[1])
    go_up(*up_new)
    arrive(5)
    cross(lower_half, upper_half)

    when(has_low, down + paces[:1], "wait_send")
    when(has_high, up + paces[1:], "wait_send")
    for copy in row_moves + swaps:
        copy.wait_send()

    def heard(k, carry):
        send_length(k).wait_send()
        send_length(k).wait_recv()
        return carry

    hand_over = remote(gathered, lengths, sum_send.at[7], sum_recv.at[7], to_partner)

    @pl.when(core == 1)
    def _():
        lax.fori_loop(1, count, heard, 0)
        hand_over.start()
        lengths[...] = gathered[...]

    pl.when(core == 0)(hand_over.wait_recv)

    owner = lax.broadcasted_iota(jnp.int32, (count, 1, LANES), 0)
    spot = lax.broadcasted_iota(jnp.int32, (count, 1, LANES), 2)
    index = OWN * owner + spot
    squares = lengths[...]
    before = jnp.concatenate([squares[count - 1 :], squares[: count - 1]], axis=0)
    halves = jnp.where(spot == 0, squares, 0.0) + jnp.where(spot == OWN, before, 0.0)
    squares = jnp.where(spot == 0, jnp.sum(halves, axis=2, keepdims=True), squares)
    segs = jnp.where((spot < OWN) & (index > 0), jnp.sqrt(squares + EPSILON), 0.0)

    def add_up(a):
        return jnp.sum(jnp.sum(a, axis=0), axis=1, keepdims=True)

    given_load.wait()
    length = add_up(segs)
    weights = []
    for i in range(OWN):
        base = bracket[i]
        arc = add_up(jnp.where(index <= base, segs, 0.0))
        seg = add_up(jnp.where(index == base + 1, segs, 0.0))
        target = length * (OWN * img + i).astype(jnp.float32) / jnp.float32(last)
        weights.append(jnp.broadcast_to((target - arc) / seg, (SUB, half)))

    for t in range(TILES):
        when(has_high, [down_new[0][t], down_new[1][t]], "wait_recv")
        when(has_low, [up_new[t]], "wait_recv")
        for i in range(OWN):
            pick = jnp.clip(bracket[i] - (OWN * img - 2), 0, 7)
            for c in chunks:
                span = slice(c, c + half)
                base = phi2[t][pick, :, span]
                out[i, t, :, span] = base + weights[i] * (phi2[t][pick + 1, :, span] - base)

    when(has_low, down_new[0] + down_new[1], "wait_send")
    when(has_high, up_new, "wait_send")
    pl.when(core == 1)(hand_over.wait_send)


def per_device(count, path, bracket):
    images, rows, cols = path.shape
    f32 = jnp.float32
    dma = pltpu.SemaphoreType.DMA
    tiled = path.reshape(images, TILES, SUB, cols)

    def slabs(number, tiles=EXT):
        return pltpu.VMEM((number, tiles, SUB, cols), f32)

    def small(*dims):
        return pltpu.VMEM((*dims, SUB, LANES), f32)

    out = pl.pallas_call(
        functools.partial(kernel, count),
        out_shape=jax.ShapeDtypeStruct((images, TILES, SUB, cols), f32),
        in_specs=[pl.BlockSpec(memory_space=pltpu.HBM), pl.BlockSpec(memory_space=pltpu.HBM)],
        out_specs=pl.BlockSpec(memory_space=pltpu.VMEM),
        scratch_shapes=[
            slabs(8),
            slabs(10),
            *[pltpu.VMEM((9, SUB, cols), f32) for _ in range(TILES)],
            slabs(6),
            slabs(8),
            slabs(8, 2),
            slabs(10, 2),
            small(6, 2), small(6, 2),
            small(6, 2), small(6, 2),
            small(OWN + 1), small(OWN + 1),
            small(6), small(8),
            pltpu.VMEM((1, 1, LANES), f32),
            pltpu.VMEM((count, 1, LANES), f32),
            pltpu.VMEM((count, 1, LANES), f32),
            dma((OWN,)),
            dma((6,)), dma((6,)), dma((6,)), dma((6,)),
            dma((24,)), dma((24,)),
            dma((8,)), dma((8,)),
            dma((3, TILES)), dma((3, TILES)),
            dma((2,)), dma((2,)),
            dma((count,)), dma((count,)),
            pltpu.SMEM((images,), jnp.int32), dma,
            pltpu.SemaphoreType.REGULAR((8,)),
        ],
        compiler_params=pltpu.CompilerParams(
            collective_id=0, has_side_effects=True, vmem_limit_bytes=40 * 1024 * 1024
        ),
    )(*(pltpu.with_memory_space_constraint(a, pltpu.HBM) for a in (tiled, bracket)))
    return out.reshape(images, rows, cols)


def solution(mesh):
    count = mesh.shape["img"]
    return jax.shard_map(
        functools.partial(per_device, count),
        mesh=mesh,
        in_specs=(P(("groups", "img"), "space", None), P(("groups", "img"))),
        out_specs=P(("groups", "img"), "space", None),
        check_vma=False,
    )
```

```python
import functools

import jax
import jax.numpy as jnp
from jax import lax
from jax.experimental import pallas as pl
from jax.experimental.pallas import tpu as pltpu
from jax.sharding import PartitionSpec as P

REACH = 2
ITERS = 2
TIME_STEP = 0.002
EPSILON = 1e-06

LANES = 128
SUB = 8
OWN = 4
TILES = 4
EXT = TILES + 1
FIRST = 4


def fold(block):
    parts = [block[:, i : i + LANES] for i in range(0, block.shape[1], LANES)]
    while len(parts) > 1:
        parts = [a + b for a, b in zip(parts[::2], parts[1::2])] + parts[len(parts) // 2 * 2 :]
    return parts[0]


def spread(vector, width):
    return jnp.concatenate([vector] * (width // LANES), axis=1)


def kernel(count, path, given, out, phi0, phi1, phi2_0, phi2_1, phi2_2, phi2_3, th0, th1, rows0, rows1,
           mine0, theirs0, mine1, theirs1, mine2, theirs2, speed0, speed1, message, gathered, lengths,
           local_sem, side_send, down_recv, up_recv, row_send, row_recv, sum_send, sum_recv,
           new_send, new_recv, pace_send, pace_recv, len_sem, bracket, given_sem, live):
    cols = path.shape[-1]
    half = min(cols, 1024)
    phi2 = (phi2_0, phi2_1, phi2_2, phi2_3)
    img = lax.axis_index("img")
    core = lax.axis_index("space")

    low = lax.rem(img + count - 1, count)
    high = lax.rem(img + 1, count)
    partner = 1 - core
    to_low, to_high, to_partner = {"img": low}, {"img": high}, {"space": partner}
    mesh_id = pl.DeviceIdType.MESH

    def remote(src, dst, send, recv, where):
        return pltpu.make_async_remote_copy(
            src_ref=src, dst_ref=dst, send_sem=send, recv_sem=recv, device_id=where, device_id_type=mesh_id
        )

    def take(ref, sem):
        remote(ref, ref, sem, sem, to_partner).wait_recv()

    p0, p1, p2, t0, t1 = (lambda w, s=s: w - s for s in (2, 1, 2, 3, 2))

    loads = [
        pltpu.make_async_copy(path.at[i], phi0.at[p0(FIRST + i), pl.ds(0, TILES)], local_sem.at[i]) for i in range(OWN)
    ]
    for i in (0, 3, 1, 2):
        loads[i].start()
    given_load = pltpu.make_async_copy(given, bracket, given_sem)
    given_load.start()

    barrier = pltpu.get_barrier_semaphore()
    def signal(sem, where):
        pl.semaphore_signal(sem, inc=1, device_id=where, device_id_type=mesh_id)

    has_low, has_high = img > 0, img < count - 1
    pl.when(has_low)(lambda: signal(barrier, to_low))
    pl.when(has_high)(lambda: signal(barrier, to_high))
    neighbours = has_low.astype(jnp.int32) + has_high.astype(jnp.int32)
    pl.semaphore_wait(barrier, neighbours + (1 - core))
    signal(barrier, to_partner)

    def when(condition, copies, act):
        @pl.when(condition)
        def _():
            for copy in copies:
                getattr(copy, act)()

    def part(ref, slot, first=0, number=TILES):
        return ref.at[slot, pl.ds(first, number)]

    def shift(ref, name, source, target, k, where, first=0, number=TILES):
        send, recv = (side_send.at[0], down_recv) if where is to_low else (side_send.at[1], up_recv)
        return remote(part(ref, name(source), first, number), part(ref, name(target), first, number),
                      send, recv.at[k], where)

    down = [
        shift(phi0, p0, 4, 8, 0, to_low), shift(phi0, p0, 5, 9, 1, to_low),
        shift(phi1, p1, 5, 9, 2, to_low), shift(phi1, p1, 4, 8, 3, to_low),
        shift(phi1, p1, 6, 10, 4, to_low, 2, 2), shift(phi1, p1, 6, 10, 5, to_low, 0, 2),
    ]
    up = [
        shift(phi0, p0, 7, 3, 0, to_high), shift(phi0, p0, 6, 2, 1, to_high),
        shift(phi1, p1, 6, 2, 2, to_high), shift(phi1, p1, 7, 3, 3, to_high),
        shift(phi1, p1, 5, 1, 4, to_high, 0, 2), shift(phi1, p1, 5, 1, 5, to_high, 2, 2),
    ]
    down_new = [
        [remote(phi2[t].at[p2(source)], phi2[t].at[p2(target)], new_send.at[0], new_recv.at[0, t], to_low)
         for t in range(TILES)]
        for source, target in ((5, 9), (6, 10))
    ]
    up_new = [
        remote(phi2[t].at[p2(6)], phi2[t].at[p2(2)], new_send.at[1], new_recv.at[1, t], to_high)
        for t in range(TILES)
    ]

    def go_down(*copies):
        when(has_low, copies, "start")

    def go_up(*copies):
        when(has_high, copies, "start")

    groups = []

    def send_rows(ref, rows, slots):
        n = len(groups)
        groups.append(rows.at[pl.ds(0, len(slots))])
        for slot in slots:
            for k, tile in enumerate((0, TILES - 1)):
                remote(ref.at[slot, tile], rows.at[slot, k], row_send.at[n], row_recv.at[n], to_partner).start()

    def halos(ref, rows, slots):
        n = len(groups) - 1
        take(groups[n], row_recv.at[n])
        for slot in slots:
            for c in chunks:
                ref[slot, TILES, :, c : c + half] = jnp.where(
                    sub < SUB // 2, rows[slot, 0, :, c : c + half], rows[slot, 1, :, c : c + half]
                )

    sub = lax.broadcasted_iota(jnp.int32, (SUB, half), 0)
    chunks = range(0, cols, half)

    for i in (0, 3, 1, 2):
        loads[i].wait()
        if i < 2:
            go_down(down[i])
        else:
            go_up(up[3 - i])
    pl.when(core == 1)(lambda: pl.semaphore_wait(barrier, 1))
    own_slots = [p0(image) for image in range(FIRST, FIRST + OWN)]
    send_rows(phi0, rows0, own_slots)
    lives = []
    while 2 ** len(lives) < count - 1:
        lives.append(2 ** len(lives))

    def say_live(n):
        for where in (img - lives[n], img + lives[n]):
            pl.when((where >= 0) & (where < count))(lambda where=where: signal(live.at[n], {"img": where}))

    def hear_live(n):
        below, above = img >= lives[n], img < count - lives[n]
        pl.semaphore_wait(live.at[n], below.astype(jnp.int32) + above.astype(jnp.int32))

    if lives:
        say_live(0)

    is_first = (img == 0).astype(jnp.int32)
    is_last = (img == count - 1).astype(jnp.int32)
    last = OWN * count - 1

    def same(image, k):
        return jnp.asarray(image == k).astype(jnp.int32)

    def sides(image):
        at_first = is_first * same(image, FIRST)
        at_last = is_last * same(image, FIRST + OWN - 1)
        end = (at_first + at_last).astype(jnp.float32)
        return image - 1 + at_first, image + 1 - at_last, (1.0 + end) * jnp.float32(last / 2.0)

    def around(ref, slot, tile, c):
        above = lax.rem(tile + EXT - 1, EXT)
        below = lax.rem(tile + 1, EXT)
        here = ref[slot, tile, :, c : c + half]
        up_rows = pltpu.roll(jnp.where(sub == SUB - 1, ref[slot, above, :, c : c + half], here), 1, 0)
        down_rows = pltpu.roll(jnp.where(sub == 0, ref[slot, below, :, c : c + half], here), SUB - 1, 0)
        if half == cols:
            left = pltpu.roll(here, 1, 1)
            right = pltpu.roll(here, half - 1, 1)
        else:
            before = (c - LANES) % cols
            after = (c + half) % cols
            wide = jnp.concatenate(
                [ref[slot, tile, :, before : before + LANES], here, ref[slot, tile, :, after : after + LANES]], axis=1
            )
            left = pltpu.roll(wide, 1, 1)[:, LANES : LANES + half]
            right = pltpu.roll(wide, half + 2 * LANES - 1, 1)[:, LANES : LANES + half]
        return here, (up_rows + down_rows) + (left + right) - 4.0 * here

    zero = jnp.zeros((SUB, LANES), jnp.float32)

    def over(tiles, one, init):
        first, end = tiles
        return lax.fori_loop(first, end, one, init)

    full, slab, upper_half, lower_half = (0, EXT), (0, TILES), (0, 2), (2, TILES)

    def drift(phi, th, slot, th_slot, tiles, total=None):
        def one(tile, acc):
            for c in chunks:
                here, lap = around(phi, slot, tile, c)
                force = lap + here - here * here * here
                th[th_slot, tile, :, c : c + half] = force
                acc = acc + jnp.where(tile < TILES, fold(force * force), 0.0)
            return acc

        acc = over(tiles, one, zero)
        if total is not None:
            total[...] = acc

    def stretch_sum(phi, lower, upper, total, factor):
        def one(tile, acc):
            for c in chunks:
                gap = phi[upper, tile, :, c : c + half] - phi[lower, tile, :, c : c + half]
                acc = acc + fold(gap * gap)
            return acc

        total[...] = over(slab, one, zero) * (factor * factor)

    def segment_sum(image, total, tiles=range(TILES)):
        acc = zero
        for t in tiles:
            for c in chunks:
                gap = phi2[t][p2(image), :, c : c + half] - phi2[t][p2(image - 1), :, c : c + half]
                acc = acc + fold(gap * gap)
        total[...] = acc

    def theta(phi, th, lower, upper, factor, th_slot, speed, tiles):
        scale = spread(speed * factor, half)

        def one(tile, carry):
            for c in chunks:
                span = slice(c, c + half)
                gap = phi[upper, tile, :, span] - phi[lower, tile, :, span]
                th[th_slot, tile, :, span] = scale * gap - th[th_slot, tile, :, span]
            return carry

        over(tiles, one, 0)

    def advance(phi, slot, th, th_slot, new, new_slot, speed, image, tiles):
        fixed = is_first * same(image, FIRST) + is_last * same(image, FIRST + OWN - 1)
        scale = spread(speed * jnp.float32(last / 2.0), half)

        def one(tile, carry):
            for c in chunks:
                span = slice(c, c + half)
                here, lap = around(th, th_slot, tile, c)
                old = phi[slot, tile, :, span]
                bend = th[th_slot + 1, tile, :, span] - th[th_slot - 1, tile, :, span]
                descent = scale * bend + lap + (1.0 - 3.0 * old * old) * here
                value = jnp.where(fixed == 0, old + TIME_STEP * descent, old)
                if new is phi2:
                    new[tile][new_slot, :, span] = value
                else:
                    new[new_slot, tile, :, span] = value
            return carry

        if new is phi2:
            for tile in range(*tiles):
                one(tile, 0)
        else:
            over(tiles, one, 0)

    def whole(a):
        return jnp.broadcast_to(jnp.sum(jnp.sum(a, axis=1, keepdims=True), axis=0, keepdims=True), (SUB, LANES))

    def speeds(mine, theirs, first, number, out_ref):
        for i in range(first, first + number):
            force = whole(mine[i, 0] + theirs[i, 0])
            stretch = whole(mine[i, 1] + theirs[i, 1])
            out_ref[i] = jnp.sqrt(force + EPSILON) / jnp.sqrt(stretch + EPSILON)

    def place(image):
        if isinstance(image, int):
            return 2 * (5 - image) if image < 6 else 2 * (image - 6) + 1
        return jnp.where(image < 6, 2 * (5 - image), 2 * (image - 6) + 1)

    def each(images, body):
        start, step, number = images

        def one(i, carry):
            body(start + step * i)
            return carry

        lax.fori_loop(0, number, one, 0)

    every, mids, ends, outs = (4, 1, 4), (5, 1, 2), (4, 3, 2), (3, 5, 2)

    def gap0(image):
        lower, upper, factor = sides(image)
        stretch_sum(phi0, p0(lower), p0(upper), mine0.at[place(image), 1], factor)

    def drift0(image):
        drift(phi0, th0, p0(image), t0(image), full, mine0.at[place(image), 0])

    def theta0(image):
        lower, upper, factor = sides(image)
        theta(phi0, th0, p0(lower), p0(upper), factor, t0(image), speed0[place(image)], full)

    def next1(image):
        advance(phi0, p0(image), th0, t0(image), phi1, p1(image), speed0[place(image)], image, full)

    def gap1(image):
        lower, upper, factor = sides(image)
        stretch_sum(phi1, p1(lower), p1(upper), mine1.at[place(image), 1], factor)

    def drift1(image):
        drift(phi1, th1, p1(image), t1(image), full, mine1.at[place(image), 0])

    def theta1(image, tiles=full):
        lower, upper, factor = sides(image)
        theta(phi1, th1, p1(lower), p1(upper), factor, t1(image), speed1[place(image)], tiles)

    def next2(image, tiles=slab):
        advance(phi1, p1(image), th1, t1(image), phi2, p2(image), speed1[place(image)], image, tiles)

    swaps = []

    def exchange(mine, theirs, first, number):
        k = len(swaps)
        span = pl.ds(first, number)
        move = remote(mine.at[span], theirs.at[span], sum_send.at[k], sum_recv.at[k], to_partner)
        move.start()
        swaps.append(move)
        return move

    def arrive(k):
        when(has_high, [down[k]], "wait_recv")
        when(has_low, [up[k]], "wait_recv")

    def live_round(n):
        if n < len(lives):
            hear_live(n)
            if n + 1 < len(lives):
                say_live(n + 1)

    halos(phi0, rows0, own_slots)
    live_round(0)
    each(every, drift0)
    each(mids, gap0)
    live_round(1)

    arrive(0)
    slots = [p0(image) for image in (3, 8)]
    send_rows(phi0, rows0, slots)
    each(ends, gap0)
    move = exchange(mine0, theirs0, 0, OWN)
    halos(phi0, rows0, slots)
    move.wait_recv()
    speeds(mine0, theirs0, 0, OWN, speed0)
    each(every, theta0)
    each(mids, next1)
    go_down(down[2])
    go_up(up[2])
    each(outs, drift0)
    each(mids, drift1)
    live_round(2)

    arrive(1)
    slots = [p0(image) for image in (2, 9)]
    send_rows(phi0, rows0, slots)
    each(outs, gap0)
    move = exchange(mine0, theirs0, OWN, 2)
    halos(phi0, rows0, slots)
    move.wait_recv()
    speeds(mine0, theirs0, OWN, 2, speed0)
    each(outs, theta0)
    each(ends, next1)
    go_down(down[3])
    go_up(up[3])
    each(mids, gap1)
    move = exchange(mine1, theirs1, 0, 2)
    each(ends, drift1)
    move.wait_recv()
    speeds(mine1, theirs1, 0, 2, speed1)
    paces = [
        remote(speed1.at[0], speed1.at[7], pace_send.at[0], pace_recv.at[0], to_low),
        remote(speed1.at[1], speed1.at[6], pace_send.at[1], pace_recv.at[1], to_high),
    ]
    each(mids, theta1)
    go_down(paces[0], *down[4:6])
    go_up(paces[1], *up[4:6])
    live_round(3)

    arrive(2)
    slots = [p1(image) for image in (2, 9)]
    send_rows(phi1, rows1, slots)
    each(outs, gap1)
    halos(phi1, rows1, slots)
    for image in (2, 9):
        drift(phi1, th1, p1(image), t1(image), slab)

    arrive(3)
    slots = [p1(image) for image in (3, 8)]
    send_rows(phi1, rows1, slots)
    each(ends, gap1)
    move = exchange(mine1, theirs1, 2, 2)
    halos(phi1, rows1, slots)
    each(outs, drift1)
    last_move = exchange(mine1, theirs1, 4, 2)
    move.wait_recv()
    speeds(mine1, theirs1, 2, 2, speed1)
    each(ends, theta1)
    each(mids, next2)
    last_move.wait_recv()
    speeds(mine1, theirs1, 4, 2, speed1)
    each(outs, theta1)
    each(ends, next2)
    for image in (5, 6, 7):
        segment_sum(image, mine2.at[image - FIRST])

    when(has_high, [paces[0]], "wait_recv")
    when(has_low, [paces[1]], "wait_recv")
    arrive(4)

    def cross(low_tiles, high_tiles):
        theta1(2, low_tiles)
        theta1(9, high_tiles)
        next2(3, low_tiles)
        next2(8, high_tiles)

    cross(upper_half, lower_half)
    segment_sum(4, mine2.at[0], range(*upper_half))
    segment_sum(8, mine2.at[OWN], range(*lower_half))
    move = exchange(mine2, theirs2, 0, OWN + 1)
    move.wait_recv()

    lane = lax.broadcasted_iota(jnp.int32, (1, LANES), 1)
    squares = jnp.zeros((1, LANES), jnp.float32)
    for i in range(OWN + 1):
        squares = jnp.where(lane == i, whole(mine2[i] + theirs2[i])[0:1], squares)
    message[0] = squares
    gathered[img] = squares

    live_round(4)

    def send_length(k):
        return remote(message.at[0], gathered.at[img], len_sem.at[0], len_sem.at[1], {"img": lax.rem(img + k, count)})

    def spread_out(i, carry):
        distance = count // 2 - 1 - i
        send_length(distance).start()
        send_length(count - distance).start()
        return carry

    @pl.when(core == 1)
    def _():
        send_length(count // 2).start()
        lax.fori_loop(0, count // 2 - 1, spread_out, 0)

    go_down(*down_new[0], *down_new[1])
    go_up(*up_new)
    arrive(5)
    cross(lower_half, upper_half)

    crossed = part(phi1, pl.ds(0, 5))
    pl.when(has_low)(lambda: take(crossed, side_send.at[0]))
    pl.when(has_high)(lambda: take(crossed, side_send.at[1]))
    when(has_low, paces[:1], "wait_send")
    when(has_high, paces[1:], "wait_send")
    for n, group in enumerate(groups):
        take(group, row_send.at[n])
    for copy in swaps:
        copy.wait_send()

    hand_over = remote(gathered, lengths, sum_send.at[6], sum_recv.at[6], to_partner)

    @pl.when(core == 1)
    def _():
        others = gathered.at[pl.ds(0, count - 1)]
        take(others, len_sem.at[0])
        take(others, len_sem.at[1])
        hand_over.start()
        lengths[...] = gathered[...]

    pl.when(core == 0)(hand_over.wait_recv)

    owner = lax.broadcasted_iota(jnp.int32, (count, 1, LANES), 0)
    spot = lax.broadcasted_iota(jnp.int32, (count, 1, LANES), 2)
    index = OWN * owner + spot
    squares = lengths[...]
    before = jnp.concatenate([squares[count - 1 :], squares[: count - 1]], axis=0)
    halves = jnp.where(spot == 0, squares, 0.0) + jnp.where(spot == OWN, before, 0.0)
    squares = jnp.where(spot == 0, jnp.sum(halves, axis=2, keepdims=True), squares)
    segs = jnp.where((spot < OWN) & (index > 0), jnp.sqrt(squares + EPSILON), 0.0)

    def add_up(a):
        return jnp.sum(jnp.sum(a, axis=0), axis=1, keepdims=True)

    given_load.wait()
    length = add_up(segs)
    weights = []
    for i in range(OWN):
        base = bracket[i]
        arc = add_up(jnp.where(index <= base, segs, 0.0))
        seg = add_up(jnp.where(index == base + 1, segs, 0.0))
        target = length * (OWN * img + i).astype(jnp.float32) / jnp.float32(last)
        weights.append(jnp.broadcast_to((target - arc) / seg, (SUB, half)))

    for t in range(TILES):
        pl.when(has_high)(lambda t=t: take(phi2[t].at[pl.ds(0, 2)], new_recv.at[0, t]))
        when(has_low, [up_new[t]], "wait_recv")
        for i in range(OWN):
            pick = jnp.clip(bracket[i] - (OWN * img - 2), 0, 7)
            for c in chunks:
                span = slice(c, c + half)
                base = phi2[t][pick, :, span]
                out[i, t, :, span] = base + weights[i] * (phi2[t][pick + 1, :, span] - base)

    pl.when(has_low)(lambda: take(part(phi1, pl.ds(0, 2)), new_send.at[0]))
    pl.when(has_high)(lambda: take(part(phi1, 0), new_send.at[1]))
    pl.when(core == 1)(hand_over.wait_send)


def per_device(count, path, bracket):
    images, rows, cols = path.shape
    f32 = jnp.float32
    dma = pltpu.SemaphoreType.DMA
    tiled = path.reshape(images, TILES, SUB, cols)

    def slabs(number, tiles=EXT):
        return pltpu.VMEM((number, tiles, SUB, cols), f32)

    def small(*dims):
        return pltpu.VMEM((*dims, SUB, LANES), f32)

    out = pl.pallas_call(
        functools.partial(kernel, count),
        out_shape=jax.ShapeDtypeStruct((images, TILES, SUB, cols), f32),
        in_specs=[pl.BlockSpec(memory_space=pltpu.HBM), pl.BlockSpec(memory_space=pltpu.HBM)],
        out_specs=pl.BlockSpec(memory_space=pltpu.VMEM),
        scratch_shapes=[
            slabs(8),
            slabs(10),
            *[pltpu.VMEM((9, SUB, cols), f32) for _ in range(TILES)],
            slabs(6),
            slabs(8),
            slabs(8, 2),
            slabs(10, 2),
            small(6, 2), small(6, 2),
            small(6, 2), small(6, 2),
            small(OWN + 1), small(OWN + 1),
            small(6), small(8),
            pltpu.VMEM((1, 1, LANES), f32),
            pltpu.VMEM((count, 1, LANES), f32),
            pltpu.VMEM((count, 1, LANES), f32),
            dma((OWN,)),
            dma((2,)), dma((6,)), dma((6,)),
            dma((5,)), dma((5,)),
            dma((7,)), dma((7,)),
            dma((2,)), dma((2, TILES)),
            dma((2,)), dma((2,)),
            dma((2,)),
            pltpu.SMEM((images,), jnp.int32), dma,
            pltpu.SemaphoreType.REGULAR((5,)),
        ],
        compiler_params=pltpu.CompilerParams(
            collective_id=0, has_side_effects=True, vmem_limit_bytes=40 * 1024 * 1024
        ),
    )(*(pltpu.with_memory_space_constraint(a, pltpu.HBM) for a in (tiled, bracket)))
    return out.reshape(images, rows, cols)


def solution(mesh):
    count = mesh.shape["img"]
    return jax.shard_map(
        functools.partial(per_device, count),
        mesh=mesh,
        in_specs=(P(("groups", "img"), "space", None), P(("groups", "img"))),
        out_specs=P(("groups", "img"), "space", None),
        check_vma=False,
    )
```

```python
import functools

import jax
import jax.numpy as jnp
from jax import lax
from jax.experimental import pallas as pl
from jax.experimental.pallas import tpu as pltpu
from jax.sharding import PartitionSpec as P

REACH = 2
ITERS = 2
TIME_STEP = 0.002
EPSILON = 1e-06

LANES = 128
SUB = 8
OWN = 4
TILES = 4
EXT = TILES + 1
FIRST = 4


def fold(block):
    parts = [block[:, i : i + LANES] for i in range(0, block.shape[1], LANES)]
    while len(parts) > 1:
        parts = [a + b for a, b in zip(parts[::2], parts[1::2])] + parts[len(parts) // 2 * 2 :]
    return parts[0]


def spread(vector, width):
    return jnp.concatenate([vector] * (width // LANES), axis=1)


def kernel(count, path, given, out, phi0, phi1, phi2_0, phi2_1, phi2_2, phi2_3, th0, th1, rows0, rows1,
           mine0, theirs0, mine1, theirs1, mine2, theirs2, speed0, speed1, message, gathered,
           local_sem, side_send, down_recv, up_recv, row_send, row_recv, sum_send, sum_recv,
           new_send, new_recv, pace_send, pace_recv, len_sem, bracket, given_sem, live):
    cols = path.shape[-1]
    half = min(cols, 1024)
    phi2 = (phi2_0, phi2_1, phi2_2, phi2_3)
    img = lax.axis_index("img")
    core = lax.axis_index("space")

    low = lax.rem(img + count - 1, count)
    high = lax.rem(img + 1, count)
    partner = 1 - core
    to_low, to_high, to_partner = {"img": low}, {"img": high}, {"space": partner}
    mesh_id = pl.DeviceIdType.MESH

    def remote(src, dst, send, recv, where):
        return pltpu.make_async_remote_copy(
            src_ref=src, dst_ref=dst, send_sem=send, recv_sem=recv, device_id=where, device_id_type=mesh_id
        )

    def take(ref, sem):
        remote(ref, ref, sem, sem, to_partner).wait_recv()

    p0, p1, p2, t0, t1 = (lambda w, s=s: w - s for s in (2, 1, 2, 3, 2))

    loads = [
        pltpu.make_async_copy(path.at[i], phi0.at[p0(FIRST + i), pl.ds(0, TILES)], local_sem.at[i]) for i in range(OWN)
    ]
    given_load = pltpu.make_async_copy(given, bracket, given_sem)

    barrier = pltpu.get_barrier_semaphore()
    def signal(sem, where):
        pl.semaphore_signal(sem, inc=1, device_id=where, device_id_type=mesh_id)

    has_low, has_high = img > 0, img < count - 1
    pl.when(has_low)(lambda: signal(barrier, to_low))
    pl.when(has_high)(lambda: signal(barrier, to_high))
    for i in (0, 3, 1, 2):
        loads[i].start()
    given_load.start()
    neighbours = has_low.astype(jnp.int32) + has_high.astype(jnp.int32)
    pl.semaphore_wait(barrier, neighbours + (1 - core))
    signal(barrier, to_partner)

    def when(condition, copies, act):
        @pl.when(condition)
        def _():
            for copy in copies:
                getattr(copy, act)()

    def part(ref, slot, first=0, number=TILES):
        return ref.at[slot, pl.ds(first, number)]

    def shift(ref, name, source, target, k, where, first=0, number=TILES):
        send, recv = (side_send.at[0], down_recv) if where is to_low else (side_send.at[1], up_recv)
        return remote(part(ref, name(source), first, number), part(ref, name(target), first, number),
                      send, recv.at[k], where)

    down = [
        shift(phi0, p0, 4, 8, 0, to_low), shift(phi0, p0, 5, 9, 1, to_low),
        shift(phi1, p1, 5, 9, 2, to_low), shift(phi1, p1, 4, 8, 3, to_low),
        shift(phi1, p1, 6, 10, 4, to_low, 2, 2), shift(phi1, p1, 6, 10, 5, to_low, 0, 2),
    ]
    up = [
        shift(phi0, p0, 7, 3, 0, to_high), shift(phi0, p0, 6, 2, 1, to_high),
        shift(phi1, p1, 6, 2, 2, to_high), shift(phi1, p1, 7, 3, 3, to_high),
        shift(phi1, p1, 5, 1, 4, to_high, 0, 2), shift(phi1, p1, 5, 1, 5, to_high, 2, 2),
    ]
    down_new = [
        [remote(phi2[t].at[p2(source)], phi2[t].at[p2(target)], new_send.at[0], new_recv.at[0, t], to_low)
         for t in range(TILES)]
        for source, target in ((5, 9), (6, 10))
    ]
    up_new = [
        remote(phi2[t].at[p2(6)], phi2[t].at[p2(2)], new_send.at[1], new_recv.at[1, t], to_high)
        for t in range(TILES)
    ]

    def go_down(*copies):
        when(has_low, copies, "start")

    def go_up(*copies):
        when(has_high, copies, "start")

    groups = []

    def send_rows(ref, rows, slots):
        n = len(groups)
        groups.append(rows.at[pl.ds(0, len(slots))])
        for slot in slots:
            for k, tile in enumerate((0, TILES - 1)):
                remote(ref.at[slot, tile], rows.at[slot, k], row_send.at[n], row_recv.at[n], to_partner).start()

    def halos(ref, rows, slots):
        n = len(groups) - 1
        take(groups[n], row_recv.at[n])
        for slot in slots:
            for c in chunks:
                ref[slot, TILES, :, c : c + half] = jnp.where(
                    sub < SUB // 2, rows[slot, 0, :, c : c + half], rows[slot, 1, :, c : c + half]
                )

    sub = lax.broadcasted_iota(jnp.int32, (SUB, half), 0)
    chunks = range(0, cols, half)

    for i in (0, 3, 1, 2):
        loads[i].wait()
        if i < 2:
            go_down(down[i])
        else:
            go_up(up[3 - i])
    pl.when(core == 1)(lambda: pl.semaphore_wait(barrier, 1))
    own_slots = [p0(image) for image in range(FIRST, FIRST + OWN)]
    send_rows(phi0, rows0, own_slots)
    lives = []
    while 2 ** len(lives) < count - 1:
        lives.append(2 ** len(lives))

    def say_live(n):
        for where in (img - lives[n], img + lives[n]):
            pl.when((where >= 0) & (where < count))(lambda where=where: signal(live.at[n], {"img": where}))

    def hear_live(n):
        below, above = img >= lives[n], img < count - lives[n]
        pl.semaphore_wait(live.at[n], below.astype(jnp.int32) + above.astype(jnp.int32))

    if lives:
        say_live(0)

    is_first = (img == 0).astype(jnp.int32)
    is_last = (img == count - 1).astype(jnp.int32)
    last = OWN * count - 1

    def same(image, k):
        return jnp.asarray(image == k).astype(jnp.int32)

    def sides(image):
        at_first = is_first * same(image, FIRST)
        at_last = is_last * same(image, FIRST + OWN - 1)
        end = (at_first + at_last).astype(jnp.float32)
        return image - 1 + at_first, image + 1 - at_last, (1.0 + end) * jnp.float32(last / 2.0)

    def around(ref, slot, tile, c):
        above = lax.rem(tile + EXT - 1, EXT)
        below = lax.rem(tile + 1, EXT)
        here = ref[slot, tile, :, c : c + half]
        up_rows = pltpu.roll(jnp.where(sub == SUB - 1, ref[slot, above, :, c : c + half], here), 1, 0)
        down_rows = pltpu.roll(jnp.where(sub == 0, ref[slot, below, :, c : c + half], here), SUB - 1, 0)
        if half == cols:
            left = pltpu.roll(here, 1, 1)
            right = pltpu.roll(here, half - 1, 1)
        else:
            before = (c - LANES) % cols
            after = (c + half) % cols
            wide = jnp.concatenate(
                [ref[slot, tile, :, before : before + LANES], here, ref[slot, tile, :, after : after + LANES]], axis=1
            )
            left = pltpu.roll(wide, 1, 1)[:, LANES : LANES + half]
            right = pltpu.roll(wide, half + 2 * LANES - 1, 1)[:, LANES : LANES + half]
        return here, (up_rows + down_rows) + (left + right) - 4.0 * here

    zero = jnp.zeros((SUB, LANES), jnp.float32)

    def over(tiles, one, init):
        first, end = tiles
        return lax.fori_loop(first, end, one, init)

    full, slab, upper_half, lower_half = (0, EXT), (0, TILES), (0, 2), (2, TILES)

    def drift(phi, th, slot, th_slot, tiles, total=None):
        def one(tile, acc):
            for c in chunks:
                here, lap = around(phi, slot, tile, c)
                force = lap + here - here * here * here
                th[th_slot, tile, :, c : c + half] = force
                acc = acc + jnp.where(tile < TILES, fold(force * force), 0.0)
            return acc

        acc = over(tiles, one, zero)
        if total is not None:
            total[...] = acc

    def stretch_sum(phi, lower, upper, total, factor):
        def one(tile, acc):
            for c in chunks:
                gap = phi[upper, tile, :, c : c + half] - phi[lower, tile, :, c : c + half]
                acc = acc + fold(gap * gap)
            return acc

        total[...] = over(slab, one, zero) * (factor * factor)

    def segment_sum(image, total, tiles=range(TILES)):
        acc = zero
        for t in tiles:
            for c in chunks:
                gap = phi2[t][p2(image), :, c : c + half] - phi2[t][p2(image - 1), :, c : c + half]
                acc = acc + fold(gap * gap)
        total[...] = acc

    def theta(phi, th, lower, upper, factor, th_slot, speed, tiles):
        scale = spread(speed * factor, half)

        def one(tile, carry):
            for c in chunks:
                span = slice(c, c + half)
                gap = phi[upper, tile, :, span] - phi[lower, tile, :, span]
                th[th_slot, tile, :, span] = scale * gap - th[th_slot, tile, :, span]
            return carry

        over(tiles, one, 0)

    def advance(phi, slot, th, th_slot, new, new_slot, speed, image, tiles):
        fixed = is_first * same(image, FIRST) + is_last * same(image, FIRST + OWN - 1)
        scale = spread(speed * jnp.float32(last / 2.0), half)

        def one(tile, carry):
            for c in chunks:
                span = slice(c, c + half)
                here, lap = around(th, th_slot, tile, c)
                old = phi[slot, tile, :, span]
                bend = th[th_slot + 1, tile, :, span] - th[th_slot - 1, tile, :, span]
                descent = scale * bend + lap + (1.0 - 3.0 * old * old) * here
                value = jnp.where(fixed == 0, old + TIME_STEP * descent, old)
                if new is phi2:
                    new[tile][new_slot, :, span] = value
                else:
                    new[new_slot, tile, :, span] = value
            return carry

        if new is phi2:
            for tile in range(*tiles):
                one(tile, 0)
        else:
            over(tiles, one, 0)

    def whole(a):
        return jnp.broadcast_to(jnp.sum(jnp.sum(a, axis=1, keepdims=True), axis=0, keepdims=True), (SUB, LANES))

    def speeds(mine, theirs, first, number, out_ref):
        for i in range(first, first + number):
            force = whole(mine[i, 0] + theirs[i, 0])
            stretch = whole(mine[i, 1] + theirs[i, 1])
            out_ref[i] = jnp.sqrt(force + EPSILON) / jnp.sqrt(stretch + EPSILON)

    def place(image):
        if isinstance(image, int):
            return 2 * (5 - image) if image < 6 else 2 * (image - 6) + 1
        return jnp.where(image < 6, 2 * (5 - image), 2 * (image - 6) + 1)

    def each(images, body):
        start, step, number = images

        def one(i, carry):
            body(start + step * i)
            return carry

        lax.fori_loop(0, number, one, 0)

    every, mids, ends, outs = (4, 1, 4), (5, 1, 2), (4, 3, 2), (3, 5, 2)

    def gap0(image):
        lower, upper, factor = sides(image)
        stretch_sum(phi0, p0(lower), p0(upper), mine0.at[place(image), 1], factor)

    def drift0(image):
        drift(phi0, th0, p0(image), t0(image), full, mine0.at[place(image), 0])

    def theta0(image):
        lower, upper, factor = sides(image)
        theta(phi0, th0, p0(lower), p0(upper), factor, t0(image), speed0[place(image)], full)

    def next1(image):
        advance(phi0, p0(image), th0, t0(image), phi1, p1(image), speed0[place(image)], image, full)

    def gap1(image):
        lower, upper, factor = sides(image)
        stretch_sum(phi1, p1(lower), p1(upper), mine1.at[place(image), 1], factor)

    def drift1(image):
        drift(phi1, th1, p1(image), t1(image), full, mine1.at[place(image), 0])

    def theta1(image, tiles=full):
        lower, upper, factor = sides(image)
        theta(phi1, th1, p1(lower), p1(upper), factor, t1(image), speed1[place(image)], tiles)

    def next2(image, tiles=slab):
        advance(phi1, p1(image), th1, t1(image), phi2, p2(image), speed1[place(image)], image, tiles)

    swaps = []

    def exchange(mine, theirs, first, number):
        k = len(swaps)
        span = pl.ds(first, number)
        move = remote(mine.at[span], theirs.at[span], sum_send.at[k], sum_recv.at[k], to_partner)
        move.start()
        swaps.append(move)
        return move

    def arrive(k):
        when(has_high, [down[k]], "wait_recv")
        when(has_low, [up[k]], "wait_recv")

    def live_round(n):
        if n < len(lives):
            hear_live(n)
            if n + 1 < len(lives):
                say_live(n + 1)

    halos(phi0, rows0, own_slots)
    live_round(0)
    each(every, drift0)
    each(mids, gap0)
    live_round(1)

    arrive(0)
    slots = [p0(image) for image in (3, 8)]
    send_rows(phi0, rows0, slots)
    each(ends, gap0)
    move = exchange(mine0, theirs0, 0, OWN)
    halos(phi0, rows0, slots)
    move.wait_recv()
    speeds(mine0, theirs0, 0, OWN, speed0)
    each(every, theta0)
    each(mids, next1)
    go_down(down[2])
    go_up(up[2])
    each(outs, drift0)
    each(mids, drift1)
    live_round(2)

    arrive(1)
    slots = [p0(image) for image in (2, 9)]
    send_rows(phi0, rows0, slots)
    each(outs, gap0)
    move = exchange(mine0, theirs0, OWN, 2)
    halos(phi0, rows0, slots)
    move.wait_recv()
    speeds(mine0, theirs0, OWN, 2, speed0)
    each(outs, theta0)
    each(ends, next1)
    go_down(down[3])
    go_up(up[3])
    each(mids, gap1)
    move = exchange(mine1, theirs1, 0, 2)
    each(ends, drift1)
    move.wait_recv()
    speeds(mine1, theirs1, 0, 2, speed1)
    paces = [
        remote(speed1.at[0], speed1.at[7], pace_send.at[0], pace_recv.at[0], to_low),
        remote(speed1.at[1], speed1.at[6], pace_send.at[1], pace_recv.at[1], to_high),
    ]
    each(mids, theta1)
    go_down(paces[0], *down[4:6])
    go_up(paces[1], *up[4:6])
    live_round(3)

    arrive(2)
    slots = [p1(image) for image in (2, 9)]
    send_rows(phi1, rows1, slots)
    each(outs, gap1)
    halos(phi1, rows1, slots)
    for image in (2, 9):
        drift(phi1, th1, p1(image), t1(image), slab)

    arrive(3)
    slots = [p1(image) for image in (3, 8)]
    send_rows(phi1, rows1, slots)
    each(ends, gap1)
    move = exchange(mine1, theirs1, 2, 2)
    halos(phi1, rows1, slots)
    each(outs, drift1)
    last_move = exchange(mine1, theirs1, 4, 2)
    move.wait_recv()
    speeds(mine1, theirs1, 2, 2, speed1)
    each(ends, theta1)
    each(mids, next2)
    last_move.wait_recv()
    speeds(mine1, theirs1, 4, 2, speed1)
    each(outs, theta1)
    each(ends, next2)
    for image in (5, 6, 7):
        segment_sum(image, mine2.at[image - FIRST])
    when(has_low & (core == 0), down_new[0], "start")
    when(has_high & (core == 0), up_new, "start")

    when(has_high, [paces[0]], "wait_recv")
    when(has_low, [paces[1]], "wait_recv")
    arrive(4)

    def cross(low_tiles, high_tiles):
        theta1(2, low_tiles)
        theta1(9, high_tiles)
        next2(3, low_tiles)
        next2(8, high_tiles)

    cross(upper_half, lower_half)
    segment_sum(4, mine2.at[0], range(*upper_half))
    segment_sum(8, mine2.at[OWN], range(*lower_half))
    move = exchange(mine2, theirs2, 0, OWN + 1)
    move.wait_recv()

    lane = lax.broadcasted_iota(jnp.int32, (1, LANES), 1)
    squares = jnp.zeros((1, LANES), jnp.float32)
    for i in range(OWN + 1):
        squares = jnp.where(lane == i, whole(mine2[i] + theirs2[i])[0:1], squares)
    message[0] = squares
    gathered[img] = squares

    live_round(4)

    def send_length(k):
        for side in (0, 1):
            remote(message.at[0], gathered.at[img], len_sem.at[side], len_sem.at[2],
                   {"img": lax.rem(img + k, count), "space": side}).start()

    def spread_out(i, carry):
        distance = count // 2 - 1 - i
        send_length(distance)
        send_length(count - distance)
        return carry

    @pl.when(core == 1)
    def _():
        send_length(count // 2)
        lax.fori_loop(0, count // 2 - 1, spread_out, 0)

    when(has_low & (core == 1), down_new[0] + down_new[1], "start")
    when(has_high & (core == 1), up_new, "start")
    arrive(5)
    cross(lower_half, upper_half)

    sent_down = part(phi1, pl.ds(0, 2))
    turn = live.at[5]

    @pl.when(core == 1)
    def _():
        pl.when(has_low)(lambda: take(sent_down, new_send.at[0]))
        signal(turn, to_partner)

    @pl.when(core == 0)
    def _():
        pl.semaphore_wait(turn, 1)
        when(has_low, down_new[1], "start")

    crossed = part(phi1, pl.ds(0, 5))
    pl.when(has_low)(lambda: take(crossed, side_send.at[0]))
    pl.when(has_high)(lambda: take(crossed, side_send.at[1]))
    when(has_low, paces[:1], "wait_send")
    when(has_high, paces[1:], "wait_send")
    for n, group in enumerate(groups):
        take(group, row_send.at[n])
    for copy in swaps:
        copy.wait_send()

    others = gathered.at[pl.ds(0, count - 1)]

    @pl.when(core == 1)
    def _():
        take(others, len_sem.at[0])
        take(others, len_sem.at[1])

    take(others, len_sem.at[2])

    owner = lax.broadcasted_iota(jnp.int32, (count, 1, LANES), 0)
    spot = lax.broadcasted_iota(jnp.int32, (count, 1, LANES), 2)
    index = OWN * owner + spot
    squares = gathered[...]
    before = jnp.concatenate([squares[count - 1 :], squares[: count - 1]], axis=0)
    halves = jnp.where(spot == 0, squares, 0.0) + jnp.where(spot == OWN, before, 0.0)
    squares = jnp.where(spot == 0, jnp.sum(halves, axis=2, keepdims=True), squares)
    segs = jnp.where((spot < OWN) & (index > 0), jnp.sqrt(squares + EPSILON), 0.0)

    def add_up(a):
        return jnp.sum(jnp.sum(a, axis=0), axis=1, keepdims=True)

    given_load.wait()
    length = add_up(segs)
    weights = []
    for i in range(OWN):
        base = bracket[i]
        arc = add_up(jnp.where(index <= base, segs, 0.0))
        seg = add_up(jnp.where(index == base + 1, segs, 0.0))
        target = length * (OWN * img + i).astype(jnp.float32) / jnp.float32(last)
        weights.append(jnp.broadcast_to((target - arc) / seg, (SUB, half)))

    for t in range(TILES):
        pl.when(has_high)(lambda t=t: take(phi2[t].at[pl.ds(0, 2)], new_recv.at[0, t]))
        when(has_low, [up_new[t]], "wait_recv")
        for i in range(OWN):
            pick = jnp.clip(bracket[i] - (OWN * img - 2), 0, 7)
            for c in chunks:
                span = slice(c, c + half)
                base = phi2[t][pick, :, span]
                out[i, t, :, span] = base + weights[i] * (phi2[t][pick + 1, :, span] - base)

    pl.when(has_low & (core == 0))(lambda: take(sent_down, new_send.at[0]))
    pl.when(has_high)(lambda: take(part(phi1, 0), new_send.at[1]))


def per_device(count, path, bracket):
    images, rows, cols = path.shape
    f32 = jnp.float32
    dma = pltpu.SemaphoreType.DMA
    tiled = path.reshape(images, TILES, SUB, cols)

    def slabs(number, tiles=EXT):
        return pltpu.VMEM((number, tiles, SUB, cols), f32)

    def small(*dims):
        return pltpu.VMEM((*dims, SUB, LANES), f32)

    out = pl.pallas_call(
        functools.partial(kernel, count),
        out_shape=jax.ShapeDtypeStruct((images, TILES, SUB, cols), f32),
        in_specs=[pl.BlockSpec(memory_space=pltpu.HBM), pl.BlockSpec(memory_space=pltpu.HBM)],
        out_specs=pl.BlockSpec(memory_space=pltpu.VMEM),
        scratch_shapes=[
            slabs(8),
            slabs(10),
            *[pltpu.VMEM((9, SUB, cols), f32) for _ in range(TILES)],
            slabs(6),
            slabs(8),
            slabs(8, 2),
            slabs(10, 2),
            small(6, 2), small(6, 2),
            small(6, 2), small(6, 2),
            small(OWN + 1), small(OWN + 1),
            small(6), small(8),
            pltpu.VMEM((1, 1, LANES), f32),
            pltpu.VMEM((count, 1, LANES), f32),
            dma((OWN,)),
            dma((2,)), dma((6,)), dma((6,)),
            dma((5,)), dma((5,)),
            dma((6,)), dma((6,)),
            dma((2,)), dma((2, TILES)),
            dma((2,)), dma((2,)),
            dma((3,)),
            pltpu.SMEM((images,), jnp.int32), dma,
            pltpu.SemaphoreType.REGULAR((6,)),
        ],
        compiler_params=pltpu.CompilerParams(
            collective_id=0, has_side_effects=True, vmem_limit_bytes=40 * 1024 * 1024
        ),
    )(*(pltpu.with_memory_space_constraint(a, pltpu.HBM) for a in (tiled, bracket)))
    return out.reshape(images, rows, cols)


def solution(mesh):
    count = mesh.shape["img"]
    return jax.shard_map(
        functools.partial(per_device, count),
        mesh=mesh,
        in_specs=(P(("groups", "img"), "space", None), P(("groups", "img"))),
        out_specs=P(("groups", "img"), "space", None),
        check_vma=False,
    )
```

```python
import functools

import jax
import jax.numpy as jnp
from jax import lax
from jax.experimental import pallas as pl
from jax.experimental.pallas import tpu as pltpu
from jax.sharding import PartitionSpec as P

REACH = 2
ITERS = 2
TIME_STEP = 0.002
EPSILON = 1e-06

LANES = 128
SUB = 8
OWN = 4
TILES = 4
EXT = TILES + 1
FIRST = 4


def fold(block):
    parts = [block[:, i : i + LANES] for i in range(0, block.shape[1], LANES)]
    while len(parts) > 1:
        parts = [a + b for a, b in zip(parts[::2], parts[1::2])] + parts[len(parts) // 2 * 2 :]
    return parts[0]


def spread(vector, width):
    return jnp.concatenate([vector] * (width // LANES), axis=1)


def kernel(count, path, given, out, phi0, phi1, phi2_0, phi2_1, phi2_2, phi2_3, th0, th1, rows0, rows1,
           mine0, theirs0, mine1, theirs1, mine2, theirs2, speed0, speed1, message, gathered,
           local_sem, side_send, down_recv, up_recv, row_send, row_recv, sum_send, sum_recv,
           new_send, new_recv, pace_send, pace_recv, len_sem, bracket, given_sem, live):
    cols = path.shape[-1]
    half = min(cols, 1024)
    phi2 = (phi2_0, phi2_1, phi2_2, phi2_3)
    img = lax.axis_index("img")
    core = lax.axis_index("space")

    low = lax.rem(img + count - 1, count)
    high = lax.rem(img + 1, count)
    partner = 1 - core
    to_low, to_high, to_partner = {"img": low}, {"img": high}, {"space": partner}
    mesh_id = pl.DeviceIdType.MESH

    def remote(src, dst, send, recv, where):
        return pltpu.make_async_remote_copy(
            src_ref=src, dst_ref=dst, send_sem=send, recv_sem=recv, device_id=where, device_id_type=mesh_id
        )

    def take(ref, sem):
        remote(ref, ref, sem, sem, to_partner).wait_recv()

    p0, p1, p2, t0, t1 = (lambda w, s=s: w - s for s in (2, 1, 2, 3, 2))

    loads = [
        pltpu.make_async_copy(path.at[i], phi0.at[p0(FIRST + i), pl.ds(0, TILES)], local_sem.at[i]) for i in range(OWN)
    ]
    given_load = pltpu.make_async_copy(given, bracket, given_sem)

    barrier = pltpu.get_barrier_semaphore()
    def signal(sem, where):
        pl.semaphore_signal(sem, inc=1, device_id=where, device_id_type=mesh_id)

    has_low, has_high = img > 0, img < count - 1
    pl.when(has_low)(lambda: signal(barrier, to_low))
    pl.when(has_high)(lambda: signal(barrier, to_high))
    for i in (0, 3, 1, 2):
        loads[i].start()
    given_load.start()
    neighbours = has_low.astype(jnp.int32) + has_high.astype(jnp.int32)
    pl.semaphore_wait(barrier, neighbours + (1 - core))
    signal(barrier, to_partner)

    def when(condition, copies, act):
        @pl.when(condition)
        def _():
            for copy in copies:
                getattr(copy, act)()

    def part(ref, slot, first=0, number=TILES):
        return ref.at[slot, pl.ds(first, number)]

    def shift(ref, name, source, target, k, where, first=0, number=TILES):
        send, recv = (side_send.at[0], down_recv) if where is to_low else (side_send.at[1], up_recv)
        return remote(part(ref, name(source), first, number), part(ref, name(target), first, number),
                      send, recv.at[k], where)

    down = [
        shift(phi0, p0, 4, 8, 0, to_low), shift(phi0, p0, 5, 9, 1, to_low),
        shift(phi1, p1, 5, 9, 2, to_low), shift(phi1, p1, 4, 8, 3, to_low),
        shift(phi1, p1, 6, 10, 4, to_low, 2, 2), shift(phi1, p1, 6, 10, 5, to_low, 0, 2),
    ]
    up = [
        shift(phi0, p0, 7, 3, 0, to_high), shift(phi0, p0, 6, 2, 1, to_high),
        shift(phi1, p1, 6, 2, 2, to_high), shift(phi1, p1, 7, 3, 3, to_high),
        shift(phi1, p1, 5, 1, 4, to_high, 0, 2), shift(phi1, p1, 5, 1, 5, to_high, 2, 2),
    ]
    down_new = [
        [remote(phi2[t].at[p2(source)], phi2[t].at[p2(target)],
                new_send.at[2 if (source, t) == (6, TILES - 1) else 0], new_recv.at[0, t], to_low)
         for t in range(TILES)]
        for source, target in ((5, 9), (6, 10))
    ]
    up_new = [
        remote(phi2[t].at[p2(6)], phi2[t].at[p2(2)], new_send.at[1], new_recv.at[1, t], to_high)
        for t in range(TILES)
    ]

    def go_down(*copies):
        when(has_low, copies, "start")

    def go_up(*copies):
        when(has_high, copies, "start")

    groups = []

    def send_rows(ref, rows, slots):
        n = len(groups)
        groups.append(rows.at[pl.ds(0, len(slots))])
        for slot in slots:
            for k, tile in enumerate((0, TILES - 1)):
                remote(ref.at[slot, tile], rows.at[slot, k], row_send.at[n], row_recv.at[n], to_partner).start()

    def halos(ref, rows, slots):
        n = len(groups) - 1
        take(groups[n], row_recv.at[n])
        for slot in slots:
            for c in chunks:
                ref[slot, TILES, :, c : c + half] = jnp.where(
                    sub < SUB // 2, rows[slot, 0, :, c : c + half], rows[slot, 1, :, c : c + half]
                )

    sub = lax.broadcasted_iota(jnp.int32, (SUB, half), 0)
    chunks = range(0, cols, half)

    for i in (0, 3, 1, 2):
        loads[i].wait()
        if i < 2:
            go_down(down[i])
        else:
            go_up(up[3 - i])
    pl.when(core == 1)(lambda: pl.semaphore_wait(barrier, 1))
    own_slots = [p0(image) for image in range(FIRST, FIRST + OWN)]
    send_rows(phi0, rows0, own_slots)
    lives = []
    while 2 ** len(lives) < count - 1:
        lives.append(2 ** len(lives))

    def say_live(n):
        for where in (img - lives[n], img + lives[n]):
            pl.when((where >= 0) & (where < count))(lambda where=where: signal(live.at[n], {"img": where}))

    def hear_live(n):
        below, above = img >= lives[n], img < count - lives[n]
        pl.semaphore_wait(live.at[n], below.astype(jnp.int32) + above.astype(jnp.int32))

    if lives:
        say_live(0)

    is_first = (img == 0).astype(jnp.int32)
    is_last = (img == count - 1).astype(jnp.int32)
    last = OWN * count - 1

    def same(image, k):
        return jnp.asarray(image == k).astype(jnp.int32)

    def sides(image):
        at_first = is_first * same(image, FIRST)
        at_last = is_last * same(image, FIRST + OWN - 1)
        end = (at_first + at_last).astype(jnp.float32)
        return image - 1 + at_first, image + 1 - at_last, (1.0 + end) * jnp.float32(last / 2.0)

    def around(ref, slot, tile, c):
        above = lax.rem(tile + EXT - 1, EXT)
        below = lax.rem(tile + 1, EXT)
        here = ref[slot, tile, :, c : c + half]
        up_rows = pltpu.roll(jnp.where(sub == SUB - 1, ref[slot, above, :, c : c + half], here), 1, 0)
        down_rows = pltpu.roll(jnp.where(sub == 0, ref[slot, below, :, c : c + half], here), SUB - 1, 0)
        if half == cols:
            left = pltpu.roll(here, 1, 1)
            right = pltpu.roll(here, half - 1, 1)
        else:
            before = (c - LANES) % cols
            after = (c + half) % cols
            wide = jnp.concatenate(
                [ref[slot, tile, :, before : before + LANES], here, ref[slot, tile, :, after : after + LANES]], axis=1
            )
            left = pltpu.roll(wide, 1, 1)[:, LANES : LANES + half]
            right = pltpu.roll(wide, half + 2 * LANES - 1, 1)[:, LANES : LANES + half]
        return here, (up_rows + down_rows) + (left + right) - 4.0 * here

    zero = jnp.zeros((SUB, LANES), jnp.float32)

    def over(tiles, one, init):
        first, end = tiles
        return lax.fori_loop(first, end, one, init)

    full, slab, upper_half, lower_half = (0, EXT), (0, TILES), (0, 2), (2, TILES)

    def drift(phi, th, slot, th_slot, tiles, total=None):
        def one(tile, acc):
            for c in chunks:
                here, lap = around(phi, slot, tile, c)
                force = lap + here - here * here * here
                th[th_slot, tile, :, c : c + half] = force
                acc = acc + jnp.where(tile < TILES, fold(force * force), 0.0)
            return acc

        acc = over(tiles, one, zero)
        if total is not None:
            total[...] = acc

    def stretch_sum(phi, lower, upper, total, factor):
        def one(tile, acc):
            for c in chunks:
                gap = phi[upper, tile, :, c : c + half] - phi[lower, tile, :, c : c + half]
                acc = acc + fold(gap * gap)
            return acc

        total[...] = over(slab, one, zero) * (factor * factor)

    def segment_sum(image, total, tiles=range(TILES)):
        acc = zero
        for t in tiles:
            for c in chunks:
                gap = phi2[t][p2(image), :, c : c + half] - phi2[t][p2(image - 1), :, c : c + half]
                acc = acc + fold(gap * gap)
        total[...] = acc

    def theta(phi, th, lower, upper, factor, th_slot, speed, tiles):
        scale = spread(speed * factor, half)

        def one(tile, carry):
            for c in chunks:
                span = slice(c, c + half)
                gap = phi[upper, tile, :, span] - phi[lower, tile, :, span]
                th[th_slot, tile, :, span] = scale * gap - th[th_slot, tile, :, span]
            return carry

        over(tiles, one, 0)

    def advance(phi, slot, th, th_slot, new, new_slot, speed, image, tiles):
        fixed = is_first * same(image, FIRST) + is_last * same(image, FIRST + OWN - 1)
        scale = spread(speed * jnp.float32(last / 2.0), half)

        def one(tile, carry):
            for c in chunks:
                span = slice(c, c + half)
                here, lap = around(th, th_slot, tile, c)
                old = phi[slot, tile, :, span]
                bend = th[th_slot + 1, tile, :, span] - th[th_slot - 1, tile, :, span]
                descent = scale * bend + lap + (1.0 - 3.0 * old * old) * here
                value = jnp.where(fixed == 0, old + TIME_STEP * descent, old)
                if new is phi2:
                    new[tile][new_slot, :, span] = value
                else:
                    new[new_slot, tile, :, span] = value
            return carry

        if new is phi2:
            for tile in range(*tiles):
                one(tile, 0)
        else:
            over(tiles, one, 0)

    def whole(a):
        return jnp.broadcast_to(jnp.sum(jnp.sum(a, axis=1, keepdims=True), axis=0, keepdims=True), (SUB, LANES))

    def speeds(mine, theirs, first, number, out_ref):
        for i in range(first, first + number):
            force = whole(mine[i, 0] + theirs[i, 0])
            stretch = whole(mine[i, 1] + theirs[i, 1])
            out_ref[i] = jnp.sqrt(force + EPSILON) / jnp.sqrt(stretch + EPSILON)

    def place(image):
        if isinstance(image, int):
            return 2 * (5 - image) if image < 6 else 2 * (image - 6) + 1
        return jnp.where(image < 6, 2 * (5 - image), 2 * (image - 6) + 1)

    def each(images, body):
        start, step, number = images

        def one(i, carry):
            body(start + step * i)
            return carry

        lax.fori_loop(0, number, one, 0)

    every, mids, ends, outs = (4, 1, 4), (5, 1, 2), (4, 3, 2), (3, 5, 2)

    def gap0(image):
        lower, upper, factor = sides(image)
        stretch_sum(phi0, p0(lower), p0(upper), mine0.at[place(image), 1], factor)

    def drift0(image):
        drift(phi0, th0, p0(image), t0(image), full, mine0.at[place(image), 0])

    def theta0(image):
        lower, upper, factor = sides(image)
        theta(phi0, th0, p0(lower), p0(upper), factor, t0(image), speed0[place(image)], full)

    def next1(image):
        advance(phi0, p0(image), th0, t0(image), phi1, p1(image), speed0[place(image)], image, full)

    def gap1(image):
        lower, upper, factor = sides(image)
        stretch_sum(phi1, p1(lower), p1(upper), mine1.at[place(image), 1], factor)

    def drift1(image):
        drift(phi1, th1, p1(image), t1(image), full, mine1.at[place(image), 0])

    def theta1(image, tiles=full):
        lower, upper, factor = sides(image)
        theta(phi1, th1, p1(lower), p1(upper), factor, t1(image), speed1[place(image)], tiles)

    def next2(image, tiles=slab):
        advance(phi1, p1(image), th1, t1(image), phi2, p2(image), speed1[place(image)], image, tiles)

    swaps = []

    def exchange(mine, theirs, first, number):
        k = len(swaps)
        span = pl.ds(first, number)
        move = remote(mine.at[span], theirs.at[span], sum_send.at[k], sum_recv.at[k], to_partner)
        move.start()
        swaps.append(move)
        return move

    def arrive(k):
        when(has_high, [down[k]], "wait_recv")
        when(has_low, [up[k]], "wait_recv")

    def live_round(n):
        if n < len(lives):
            hear_live(n)
            if n + 1 < len(lives):
                say_live(n + 1)

    halos(phi0, rows0, own_slots)
    live_round(0)
    each(every, drift0)
    each(mids, gap0)
    live_round(1)

    arrive(0)
    slots = [p0(image) for image in (3, 8)]
    send_rows(phi0, rows0, slots)
    each(ends, gap0)
    move = exchange(mine0, theirs0, 0, OWN)
    halos(phi0, rows0, slots)
    move.wait_recv()
    speeds(mine0, theirs0, 0, OWN, speed0)
    each(every, theta0)
    each(mids, next1)
    go_down(down[2])
    go_up(up[2])
    each(outs, drift0)
    each(mids, drift1)
    live_round(2)

    arrive(1)
    slots = [p0(image) for image in (2, 9)]
    send_rows(phi0, rows0, slots)
    each(outs, gap0)
    move = exchange(mine0, theirs0, OWN, 2)
    halos(phi0, rows0, slots)
    move.wait_recv()
    speeds(mine0, theirs0, OWN, 2, speed0)
    each(outs, theta0)
    each(ends, next1)
    go_down(down[3])
    go_up(up[3])
    each(mids, gap1)
    move = exchange(mine1, theirs1, 0, 2)
    each(ends, drift1)
    move.wait_recv()
    speeds(mine1, theirs1, 0, 2, speed1)
    paces = [
        remote(speed1.at[0], speed1.at[7], pace_send.at[0], pace_recv.at[0], to_low),
        remote(speed1.at[1], speed1.at[6], pace_send.at[1], pace_recv.at[1], to_high),
    ]
    each(mids, theta1)
    go_down(paces[0], *down[4:6])
    go_up(paces[1], *up[4:6])
    live_round(3)

    arrive(2)
    slots = [p1(image) for image in (2, 9)]
    send_rows(phi1, rows1, slots)
    each(outs, gap1)
    halos(phi1, rows1, slots)
    for image in (2, 9):
        drift(phi1, th1, p1(image), t1(image), slab)

    arrive(3)
    slots = [p1(image) for image in (3, 8)]
    send_rows(phi1, rows1, slots)
    each(ends, gap1)
    move = exchange(mine1, theirs1, 2, 2)
    halos(phi1, rows1, slots)
    each(outs, drift1)
    last_move = exchange(mine1, theirs1, 4, 2)
    move.wait_recv()
    speeds(mine1, theirs1, 2, 2, speed1)
    each(ends, theta1)
    each(mids, next2)
    last_move.wait_recv()
    speeds(mine1, theirs1, 4, 2, speed1)
    each(outs, theta1)
    each(ends, next2)
    for image in (5, 6, 7):
        segment_sum(image, mine2.at[image - FIRST])
    when(has_low & (core == 0), down_new[0], "start")
    when(has_high & (core == 0), up_new, "start")

    when(has_high, [paces[0]], "wait_recv")
    when(has_low, [paces[1]], "wait_recv")
    arrive(4)

    def cross(low_tiles, high_tiles):
        theta1(2, low_tiles)
        theta1(9, high_tiles)
        next2(3, low_tiles)
        next2(8, high_tiles)

    cross(upper_half, lower_half)
    segment_sum(4, mine2.at[0], range(*upper_half))
    segment_sum(8, mine2.at[OWN], range(*lower_half))
    move = exchange(mine2, theirs2, 0, OWN + 1)
    move.wait_recv()

    lane = lax.broadcasted_iota(jnp.int32, (1, LANES), 1)
    squares = jnp.zeros((1, LANES), jnp.float32)
    for i in range(OWN + 1):
        squares = jnp.where(lane == i, whole(mine2[i] + theirs2[i])[0:1], squares)
    message[0] = squares
    gathered[img] = squares

    live_round(4)

    def send_length(k):
        for side in (0, 1):
            remote(message.at[0], gathered.at[img], len_sem.at[side], len_sem.at[2],
                   {"img": lax.rem(img + k, count), "space": side}).start()

    def spread_out(i, carry):
        distance = count // 2 - 1 - i
        send_length(distance)
        send_length(count - distance)
        return carry

    @pl.when(core == 1)
    def _():
        send_length(count // 2)
        lax.fori_loop(0, count // 2 - 1, spread_out, 0)

    when(has_low & (core == 1), down_new[0] + down_new[1], "start")
    when(has_high & (core == 1), up_new, "start")
    arrive(5)
    cross(lower_half, upper_half)

    sent_down = phi2[0].at[pl.ds(0, 2 * TILES - 1)]
    turn = live.at[5]

    @pl.when(core == 1)
    def _():
        pl.when(has_low)(lambda: take(sent_down, new_send.at[0]))
        signal(turn, to_partner)

    @pl.when(core == 0)
    def _():
        pl.semaphore_wait(turn, 1)
        when(has_low, down_new[1], "start")

    crossed = part(phi1, pl.ds(0, 5))
    pl.when(has_low)(lambda: take(crossed, side_send.at[0]))
    pl.when(has_high)(lambda: take(crossed, side_send.at[1]))
    when(has_low, paces[:1], "wait_send")
    when(has_high, paces[1:], "wait_send")
    for n, group in enumerate(groups):
        take(group, row_send.at[n])
    for copy in swaps:
        copy.wait_send()

    others = gathered.at[pl.ds(0, count - 1)]

    @pl.when(core == 1)
    def _():
        take(others, len_sem.at[0])
        take(others, len_sem.at[1])

    take(others, len_sem.at[2])

    owner = lax.broadcasted_iota(jnp.int32, (count, 1, LANES), 0)
    spot = lax.broadcasted_iota(jnp.int32, (count, 1, LANES), 2)
    index = OWN * owner + spot
    squares = gathered[...]
    before = jnp.concatenate([squares[count - 1 :], squares[: count - 1]], axis=0)
    halves = jnp.where(spot == 0, squares, 0.0) + jnp.where(spot == OWN, before, 0.0)
    squares = jnp.where(spot == 0, jnp.sum(halves, axis=2, keepdims=True), squares)
    segs = jnp.where((spot < OWN) & (index > 0), jnp.sqrt(squares + EPSILON), 0.0)

    def add_up(a):
        return jnp.sum(jnp.sum(a, axis=0), axis=1, keepdims=True)

    given_load.wait()
    length = add_up(segs)
    weights = []
    for i in range(OWN):
        base = bracket[i]
        arc = add_up(jnp.where(index <= base, segs, 0.0))
        seg = add_up(jnp.where(index == base + 1, segs, 0.0))
        target = length * (OWN * img + i).astype(jnp.float32) / jnp.float32(last)
        weights.append(jnp.broadcast_to((target - arc) / seg, (SUB, half)))

    for t in range(TILES):
        pl.when(has_high)(lambda t=t: take(phi2[t].at[pl.ds(0, 2)], new_recv.at[0, t]))
        when(has_low, [up_new[t]], "wait_recv")
        for i in range(OWN):
            pick = jnp.clip(bracket[i] - (OWN * img - 2), 0, 7)
            for c in chunks:
                span = slice(c, c + half)
                base = phi2[t][pick, :, span]
                out[i, t, :, span] = base + weights[i] * (phi2[t][pick + 1, :, span] - base)

    pl.when(has_low & (core == 0))(lambda: take(sent_down, new_send.at[0]))
    when(has_low, down_new[1][TILES - 1 :], "wait_send")
    pl.when(has_high)(lambda: take(part(phi1, 0), new_send.at[1]))


def per_device(count, path, bracket):
    images, rows, cols = path.shape
    f32 = jnp.float32
    dma = pltpu.SemaphoreType.DMA
    tiled = path.reshape(images, TILES, SUB, cols)

    def slabs(number, tiles=EXT):
        return pltpu.VMEM((number, tiles, SUB, cols), f32)

    def small(*dims):
        return pltpu.VMEM((*dims, SUB, LANES), f32)

    out = pl.pallas_call(
        functools.partial(kernel, count),
        out_shape=jax.ShapeDtypeStruct((images, TILES, SUB, cols), f32),
        in_specs=[pl.BlockSpec(memory_space=pltpu.HBM), pl.BlockSpec(memory_space=pltpu.HBM)],
        out_specs=pl.BlockSpec(memory_space=pltpu.VMEM),
        scratch_shapes=[
            slabs(8),
            slabs(10),
            *[pltpu.VMEM((9, SUB, cols), f32) for _ in range(TILES)],
            slabs(6),
            slabs(8),
            slabs(8, 2),
            slabs(10, 2),
            small(6, 2), small(6, 2),
            small(6, 2), small(6, 2),
            small(OWN + 1), small(OWN + 1),
            small(6), small(8),
            pltpu.VMEM((1, 1, LANES), f32),
            pltpu.VMEM((count, 1, LANES), f32),
            dma((OWN,)),
            dma((2,)), dma((6,)), dma((6,)),
            dma((5,)), dma((5,)),
            dma((6,)), dma((6,)),
            dma((3,)), dma((2, TILES)),
            dma((2,)), dma((2,)),
            dma((3,)),
            pltpu.SMEM((images,), jnp.int32), dma,
            pltpu.SemaphoreType.REGULAR((6,)),
        ],
        compiler_params=pltpu.CompilerParams(
            collective_id=0, has_side_effects=True, vmem_limit_bytes=40 * 1024 * 1024
        ),
    )(*(pltpu.with_memory_space_constraint(a, pltpu.HBM) for a in (tiled, bracket)))
    return out.reshape(images, rows, cols)


def solution(mesh):
    count = mesh.shape["img"]
    return jax.shard_map(
        functools.partial(per_device, count),
        mesh=mesh,
        in_specs=(P(("groups", "img"), "space", None), P(("groups", "img"))),
        out_specs=P(("groups", "img"), "space", None),
        check_vma=False,
    )
```
